32 devices in a mesh: pair: 2 (over core), row: 16 (over z, y, x).
Axes of the slice: x: 2, y: 2, z: 4, core: 2. Of those that a mesh axis runs over, the one named last changes fastest.
Arguments:
- snapshot: float32 [4096, 1024], P('row', 'pair'), may hold values from -6 to 6
- weights: float32 [8, 128], replicated, may hold values from 0 to 1
- block_home: int32 [8], P('pair'), may hold values from 0 to 7, each once
- plan: int32 [2, 2, 4], P(None, 'pair'), may hold values from 0 to 3, each once within a row
Outputs:
- rotated: float32 [4096, 1024], P('row', 'pair')
- column_norms: float32 [1024], P('pair')
The draws below stay inside these ranges and needn't reach their ends.
All inputs are finite; a program needn't handle non-finite values. Where the reference program divides by a largest or mean magnitude, that divisor is 1e-20 or more.
Results may differ from the reference program's by a relative error of at most 0.0001.
Values sent between devices are 32-bit elements; how exact they have to be, the bound alone decides.
No kernel may reach another device: no remote copies, remote signals or barrier semaphores. Data moves between devices by JAX's collectives and lax.ppermute only.
A program may use at most 128 MiB of HBM per device.

```python
import jax
import jax.numpy as jnp
from jax import lax

B = 128
SLOTS = 4
ROUNDS = 2
NB = 8
N = 1024
M = 4096


def block_levels(key, extent, shards, low, top_value):
    def one(dim, blocks):
        steps = jax.random.uniform(jax.random.fold_in(jax.random.fold_in(key, 6), dim), (blocks,), jnp.float32, low / len(shards), top_value / len(shards))
        return jnp.repeat(jnp.exp(steps), extent[dim] // blocks).reshape((-1,) + (1,) * (len(extent) - dim - 1))

    gain = one(*shards[0])
    for cut in shards[1:]:
        gain = gain * one(*cut)
    return gain


def normal_values(key, extent, scale, bound, pieces=(), kind=jnp.bfloat16):
    values = jax.random.normal(key, extent, jnp.float32) * scale
    if len(pieces) > 0:
        values = block_levels(key, extent, pieces, -0.22, 0.18) * values
    return jnp.clip(values, min=-bound, max=bound).astype(kind)


def setup_inputs(seed: int = 0) -> dict:
    key_of = jax.random.split(jax.random.key(seed), 5)
    return {
        "snapshot": normal_values(key_of[0], (M, N), 1.0, 6.0, ((0, 16), (1, 2)), jnp.float32),
        "weights": jnp.clip(jax.random.uniform(key_of[1], (NB, B), jnp.float32, 0.0, 1.0), 0.0, 1.0),
        "block_home": jax.random.permutation(key_of[2], NB).astype(jnp.int32),
        "plan": jax.vmap(lambda own: jax.random.permutation(own, SLOTS))(jax.random.split(key_of[3], ROUNDS * (NB // SLOTS))).reshape((ROUNDS, NB // SLOTS, SLOTS)).astype(jnp.int32),
    }


epsilon = 1e-06
step_size = 4.0
newton_turns = 5
highest = lax.Precision.HIGHEST

def rotation(gram_matrix, spread):
    diagonal_part = jnp.diagonal(gram_matrix, axis1=1, axis2=2)
    inverse = lax.rsqrt(diagonal_part + epsilon)
    corr = gram_matrix * inverse[:, :, None] * inverse[:, None, :]
    skew_part = step_size * corr * (spread[:, :, None] - spread[:, None, :])
    row_bound = 1.0 + lax.optimization_barrier(jnp.max(lax.optimization_barrier(jnp.sum(jnp.abs(skew_part), axis=2)), axis=1))
    unit_matrix = jnp.eye(gram_matrix.shape[1], dtype=jnp.float32)
    current = unit_matrix[None] + skew_part / row_bound[:, None, None]
    for index in range(newton_turns):
        inner_gram = jnp.einsum('pcd,pce->pde', current, current, precision=highest)
        current = jnp.einsum('pcd,pde->pce', current, 1.5 * unit_matrix[None] - 0.5 * inner_gram, precision=highest)
    return current

def one_group(operands):
    blocks_here, scales = operands
    row_count = blocks_here.shape[0]
    paired = jnp.transpose(blocks_here.reshape(row_count, 2, 2 * B), (1, 0, 2))
    gram_matrix = jnp.einsum('prc,prd->pcd', paired, paired, precision=highest)
    turn_matrix = rotation(gram_matrix, scales.reshape(2, 2 * B))
    result = jnp.einsum('prc,pcd->prd', paired, turn_matrix, precision=highest)
    return jnp.transpose(result, (1, 0, 2)).reshape(row_count, SLOTS, B)

def reference(snapshot, weights, block_home, plan):
    total_rows = snapshot.shape[0]
    owners = NB // SLOTS
    blocks = jnp.transpose(snapshot.reshape(total_rows, owners, SLOTS, B), (1, 0, 2, 3))
    spread = jnp.take(weights, block_home.astype(jnp.int32), axis=0).reshape(owners, SLOTS, B)
    for round_index in range(ROUNDS):
        ordering = plan[round_index].astype(jnp.int32)
        blocks = jnp.take_along_axis(blocks, ordering[:, None, :, None], axis=2)
        spread = jnp.take_along_axis(spread, ordering[:, :, None], axis=1)
        blocks = lax.map(one_group, (blocks, spread))
        blocks = jnp.stack([jnp.roll(blocks[:, :, 0], 1, axis=0), blocks[:, :, 1], blocks[:, :, 2], jnp.roll(blocks[:, :, 3], -1, axis=0)], axis=2)
        spread = jnp.stack([jnp.roll(spread[:, 0], 1, axis=0), spread[:, 1], spread[:, 2], jnp.roll(spread[:, 3], -1, axis=0)], axis=1)
    result = jnp.transpose(blocks, (1, 0, 2, 3)).reshape(total_rows, NB * B)
    column_norms = jnp.sqrt(lax.optimization_barrier(jnp.sum(result * result, axis=0)))
    return (result, column_norms)
```

```python
import jax
import jax.numpy as jnp
from jax import lax
from jax.experimental import pallas as pl
from jax.experimental.pallas import tpu as pltpu
from jax.sharding import PartitionSpec as P

epsilon = 1e-06
step_size = 4.0
newton_turns = 5
tile = 8
f32 = jnp.float32
bf16 = jnp.bfloat16

VMEM = pl.BlockSpec(memory_space=pltpu.VMEM)
SMEM = pl.BlockSpec(memory_space=pltpu.SMEM)


def split(x):
    high = x.astype(bf16)
    return high, (x - high.astype(f32)).astype(bf16)


def dot(a, b, da, db):
    return lax.dot_general(a, b, (((da,), (db,)), ((), ())), preferred_element_type=f32)


def dot3(a, b, da, db):
    return dot(a[0], b[0], da, db) + (dot(a[0], b[1], da, db) + dot(a[1], b[0], da, db))


def iotas(n):
    return (
        lax.broadcasted_iota(jnp.int32, (n, n), 0),
        lax.broadcasted_iota(jnp.int32, (n, n), 1),
    )


def column(row):
    n = row.shape[1]
    return jnp.transpose(jnp.broadcast_to(row, (n, n)))


def start_rotation(gram, row_weight):
    n = gram.shape[0]
    i, j = iotas(n)
    same = i == j
    held = jnp.where(same, gram, 0.0)
    inv_row = lax.rsqrt(jnp.sum(held, axis=0, keepdims=True) + epsilon)
    inv_col = lax.rsqrt(jnp.sum(held, axis=1, keepdims=True) + epsilon)
    corr = gram * inv_col * inv_row
    skew = step_size * corr * (column(row_weight) - row_weight)
    bound = 1.0 + jnp.max(jnp.sum(jnp.abs(skew), axis=0, keepdims=True), axis=1, keepdims=True)
    return jnp.where(same, 1.0, 0.0) + skew * (1.0 / bound)


def rotations(grams, row_weights):
    n = grams[0].shape[0]
    i, j = iotas(n)
    diag15 = jnp.where(i == j, 1.5, 0.0)
    current = [start_rotation(g, w) for g, w in zip(grams, row_weights)]
    for _ in range(newton_turns):
        parts = [split(x) for x in current]
        inner = [dot3(p, p, 1, 1) for p in parts]
        turns = [split(diag15 - 0.5 * y) for y in inner]
        current = [dot3(p, t, 1, 0) for p, t in zip(parts, turns)]
    return current


def sizes(n, rows):
    return max(tile, rows // n)


def pack_kernel(plan, snap, out, *, width):
    n, chunk = out.shape[0], out.shape[1] - tile
    i, j = iotas(width)
    held = []
    diags = []
    for p in range(2):
        ab = [
            snap[:, pl.ds(pl.multiple_of(plan[0, 0, 2 * p + h] * width, width), width)]
            for h in range(2)
        ]
        parts = split(jnp.concatenate(ab, axis=1))
        gram = dot3(parts, parts, 0, 0)
        upper = gram[:width, :width]
        lower = gram[width:, width:]
        held.append(gram[:width, width:])
        held.append(jnp.where(i <= j, upper, lower))
        diags.append(jnp.sum(jnp.where(i == j, lower, 0.0), axis=0, keepdims=True))
    extra = jnp.concatenate(diags + [jnp.zeros((tile - 2, width), f32)], axis=0)
    for c in range(n):
        start = c * chunk
        out[c, :chunk, :] = held[start // width][start % width : start % width + chunk]
        out[c, chunk:, :] = extra if c == 0 else jnp.zeros((tile, width), f32)


def sum_kernel(parts, out):
    n = parts.shape[0]
    values = [parts[c] for c in range(n)]
    while len(values) > 1:
        values = [a + b for a, b in zip(values[0::2], values[1::2])] + (
            [values[-1]] if len(values) % 2 else []
        )
    for c in range(n):
        out[c] = values[0]


def unpack(gathered, p, width):
    chunk = gathered.shape[1] - tile
    rows = []
    per = width // chunk
    for q in range(2):
        first = (2 * p + q) * per
        rows.append(jnp.concatenate([gathered[first + c, :chunk, :] for c in range(per)], axis=0))
    cross, both = rows
    i, j = iotas(width)
    flipped = jnp.transpose(both)
    diag_b = gathered[0, chunk + p : chunk + p + 1, :]
    upper = jnp.where(i <= j, both, flipped)
    lower = jnp.where(i > j, both, jnp.where(i == j, diag_b, flipped))
    return whole(upper, cross, lower)


def whole(upper, cross, lower):
    return jnp.concatenate(
        [
            jnp.concatenate([upper, cross], axis=1),
            jnp.concatenate([jnp.transpose(cross), lower], axis=1),
        ],
        axis=0,
    )


def first_kernel(plan, home, weights, snap, gathered, send, keep, *, width):
    rows = snap.shape[0]
    grams, spreads, blocks = [], [], []
    for p in range(2):
        order = [plan[0, 0, 2 * p + h] for h in range(2)]
        grams.append(unpack(gathered, p, width))
        spreads.append(
            jnp.concatenate([weights[pl.ds(home[s], 1), :] for s in order], axis=1)
        )
        blocks.append(
            jnp.concatenate(
                [snap[:, pl.ds(pl.multiple_of(s * width, width), width)] for s in order], axis=1
            )
        )
    turns = rotations(grams, spreads)
    places = [[(send, 0), (keep, 0)], [(keep, 1), (send, 1)]]
    for p in range(2):
        q = split(turns[p])
        result = dot3(split(blocks[p]), q, 1, 0)
        moved = split(dot3(split(grams[p]), q, 1, 0))
        for h in range(2):
            ref, at = places[p][h]
            cut = slice(h * width, (h + 1) * width)
            own = dot3([x[:, cut] for x in q], [x[:, cut] for x in moved], 0, 0)
            ref[at, :rows, :] = result[:, cut]
            ref[at, rows : rows + width, :] = own
            ref[at, rows + width :, :] = jnp.broadcast_to(spreads[p][:, cut], (tile, width))


def gather_slots(keep, received, held):
    held[0] = received[0]
    held[1] = keep[0]
    held[2] = keep[1]
    held[3] = received[1]


def cross_kernel(plan, keep, received, out, held, *, rows, width):
    gather_slots(keep, received, held)
    n, chunk = out.shape[0], out.shape[1]
    crosses = []
    for p in range(2):
        a, b = [split(held[plan[1, 0, 2 * p + h], :rows, :]) for h in range(2)]
        crosses.append(dot3(a, b, 0, 0))
    for c in range(n):
        start = c * chunk
        if start < 2 * width:
            out[c] = crosses[start // width][start % width : start % width + chunk]
        else:
            out[c] = jnp.zeros((chunk, width), f32)


def second_kernel(plan, keep, received, gathered, send, kept, held, *, rows, width):
    gather_slots(keep, received, held)
    chunk = gathered.shape[1]
    per = width // chunk
    grams, spreads, blocks = [], [], []
    for p in range(2):
        order = [plan[1, 0, 2 * p + h] for h in range(2)]
        cross = jnp.concatenate([gathered[p * per + c] for c in range(per)], axis=0)
        own = [held[s, rows : rows + width, :] for s in order]
        grams.append(whole(own[0], cross, own[1]))
        spreads.append(
            jnp.concatenate([held[s, rows + width : rows + width + 1, :] for s in order], axis=1)
        )
        blocks.append(jnp.concatenate([held[s, :rows, :] for s in order], axis=1))
    turns = rotations(grams, spreads)
    places = [[(send, 0), (kept, 0)], [(kept, 1), (send, 1)]]
    for p in range(2):
        q = split(turns[p])
        result = dot3(split(blocks[p]), q, 1, 0)
        moved = dot3(split(grams[p]), q, 1, 0)
        squares = jnp.sum(turns[p] * moved, axis=0, keepdims=True)
        norms = jnp.sqrt(squares)
        for h in range(2):
            ref, at = places[p][h]
            cut = slice(h * width, (h + 1) * width)
            ref[at, :rows, :] = result[:, cut]
            ref[at, rows:, :] = jnp.broadcast_to(norms[:, cut], (tile, width))


def last_kernel(kept, received, final, norms):
    rows = final.shape[0]
    width = kept.shape[2]
    order = [(received, 0), (kept, 0), (kept, 1), (received, 1)]
    for s, (ref, at) in enumerate(order):
        final[:, s * width : (s + 1) * width] = ref[at, :rows, :]
        norms[s : s + 1, :] = ref[at, rows : rows + 1, :]


def call(kernel, outs, specs, scratch=(), **static):
    def run(*refs):
        kernel(*refs, **static)

    run.__name__ = kernel.__name__
    return pl.pallas_call(
        run,
        out_shape=outs,
        in_specs=specs,
        out_specs=jax.tree.map(lambda _: VMEM, outs),
        scratch_shapes=scratch,
        name=kernel.__name__,
    )


def shape(*dims):
    return jax.ShapeDtypeStruct(dims, f32)


def exchange(send):
    count = lax.axis_size("pair")
    ahead = [((i - 1) % count, i) for i in range(count)]
    behind = [((i + 1) % count, i) for i in range(count)]
    if sorted(ahead) == sorted(behind):
        return lax.ppermute(send, "pair", ahead)
    return jnp.stack(
        [lax.ppermute(send[0], "pair", ahead), lax.ppermute(send[1], "pair", behind)]
    )


def total(parts):
    mine = lax.all_to_all(parts, "row", 0, 0, tiled=True)
    summed = call(sum_kernel, shape(*parts.shape), [VMEM])(mine)
    return lax.all_to_all(summed, "row", 0, 0, tiled=True)


def body(snapshot, weights, block_home, plan):
    rows = snapshot.shape[0]
    width = weights.shape[1]
    n = lax.axis_size("row")
    packed = call(
        pack_kernel, shape(n, sizes(n, 4 * width) + tile, width), [SMEM, VMEM], width=width
    )(plan, snapshot)
    gathered = total(packed)
    tall = rows + width + tile
    send, keep = call(
        first_kernel,
        [shape(2, tall, width), shape(2, tall, width)],
        [SMEM, SMEM, VMEM, VMEM, VMEM],
        width=width,
    )(plan, block_home, weights, snapshot, gathered)
    received = exchange(send)
    scratch = [pltpu.VMEM((4, tall, width), f32)]
    cross = call(
        cross_kernel,
        shape(n, sizes(n, 2 * width), width),
        [SMEM, VMEM, VMEM],
        scratch,
        rows=rows,
        width=width,
    )(plan, keep, received)
    gathered = total(cross)
    send, kept = call(
        second_kernel,
        [shape(2, rows + tile, width), shape(2, rows + tile, width)],
        [SMEM, VMEM, VMEM, VMEM],
        scratch,
        rows=rows,
        width=width,
    )(plan, keep, received, gathered)
    final, norms = call(
        last_kernel, [shape(rows, 4 * width), shape(4, width)], [VMEM, VMEM]
    )(kept, exchange(send))
    return final, norms.reshape(4 * width)


def solution(mesh):
    in_specs = (P("row", "pair"), P(), P("pair"), P(None, "pair", None))
    out_specs = (P("row", "pair"), P("pair"))
    return jax.shard_map(body, mesh=mesh, in_specs=in_specs, out_specs=out_specs, check_vma=False)
```

```python
import jax
import jax.numpy as jnp
from jax import lax
from jax.experimental import pallas as pl
from jax.experimental.pallas import tpu as pltpu
from jax.sharding import PartitionSpec as P

epsilon = 1e-06
step_size = 4.0
newton_turns = 5
tile = 8
grant = 16 * 1024 * 1024
f32 = jnp.float32
bf16 = jnp.bfloat16

VMEM = pl.BlockSpec(memory_space=pltpu.VMEM)
SMEM = pl.BlockSpec(memory_space=pltpu.SMEM)


def split(x):
    high = x.astype(bf16)
    return high, (x - high.astype(f32)).astype(bf16)


def dot(a, b, da, db):
    return lax.dot_general(a, b, (((da,), (db,)), ((), ())), preferred_element_type=f32)


def dot3(a, b, da, db):
    return dot(a[0], b[0], da, db) + (dot(a[0], b[1], da, db) + dot(a[1], b[0], da, db))


def iotas(n):
    return (
        lax.broadcasted_iota(jnp.int32, (n, n), 0),
        lax.broadcasted_iota(jnp.int32, (n, n), 1),
    )


def column(row):
    n = row.shape[1]
    return jnp.transpose(jnp.broadcast_to(row, (n, n)))


def start_rotation(gram, row_weight):
    n = gram.shape[0]
    i, j = iotas(n)
    same = i == j
    held = jnp.where(same, gram, 0.0)
    inv_row = lax.rsqrt(jnp.sum(held, axis=0, keepdims=True) + epsilon)
    inv_col = lax.rsqrt(jnp.sum(held, axis=1, keepdims=True) + epsilon)
    corr = gram * inv_col * inv_row
    skew = step_size * corr * (column(row_weight) - row_weight)
    bound = 1.0 + jnp.max(jnp.sum(jnp.abs(skew), axis=0, keepdims=True), axis=1, keepdims=True)
    return jnp.where(same, 1.0, 0.0) + skew * (1.0 / bound)


def rotations(grams, row_weights):
    n = grams[0].shape[0]
    i, j = iotas(n)
    diag15 = jnp.where(i == j, 1.5, 0.0)
    current = [start_rotation(g, w) for g, w in zip(grams, row_weights)]
    for _ in range(newton_turns):
        parts = [split(x) for x in current]
        inner = [dot3(p, p, 1, 1) for p in parts]
        turns = [split(diag15 - 0.5 * y) for y in inner]
        current = [dot3(p, t, 1, 0) for p, t in zip(parts, turns)]
    return current


def sizes(n, rows):
    return max(tile, rows // n)


def pack_kernel(plan, snap, out, *, width):
    n, chunk = out.shape[0], out.shape[1] - tile
    i, j = iotas(width)
    held = []
    diags = []
    for p in range(2):
        ab = [
            snap[:, pl.ds(pl.multiple_of(plan[0, 0, 2 * p + h] * width, width), width)]
            for h in range(2)
        ]
        parts = split(jnp.concatenate(ab, axis=1))
        gram = dot3(parts, parts, 0, 0)
        upper = gram[:width, :width]
        lower = gram[width:, width:]
        held.append(gram[:width, width:])
        held.append(jnp.where(i <= j, upper, lower))
        diags.append(jnp.sum(jnp.where(i == j, lower, 0.0), axis=0, keepdims=True))
    extra = jnp.concatenate(diags + [jnp.zeros((tile - 2, width), f32)], axis=0)
    for c in range(n):
        start = c * chunk
        out[c, :chunk, :] = held[start // width][start % width : start % width + chunk]
        out[c, chunk:, :] = extra if c == 0 else jnp.zeros((tile, width), f32)


def sum_kernel(parts, out):
    n = parts.shape[0]
    values = [parts[c] for c in range(n)]
    while len(values) > 1:
        values = [a + b for a, b in zip(values[0::2], values[1::2])] + (
            [values[-1]] if len(values) % 2 else []
        )
    for c in range(n):
        out[c] = values[0]


def unpack(gathered, p, width):
    chunk = gathered.shape[1] - tile
    rows = []
    per = width // chunk
    for q in range(2):
        first = (2 * p + q) * per
        rows.append(jnp.concatenate([gathered[first + c, :chunk, :] for c in range(per)], axis=0))
    cross, both = rows
    i, j = iotas(width)
    flipped = jnp.transpose(both)
    diag_b = gathered[0, chunk + p : chunk + p + 1, :]
    upper = jnp.where(i <= j, both, flipped)
    lower = jnp.where(i > j, both, jnp.where(i == j, diag_b, flipped))
    return whole(upper, cross, lower)


def whole(upper, cross, lower):
    return jnp.concatenate(
        [
            jnp.concatenate([upper, cross], axis=1),
            jnp.concatenate([jnp.transpose(cross), lower], axis=1),
        ],
        axis=0,
    )


def first_kernel(plan, home, weights, snap, gathered, send, keep, *, width):
    rows = snap.shape[0]
    grams, spreads, blocks = [], [], []
    for p in range(2):
        order = [plan[0, 0, 2 * p + h] for h in range(2)]
        grams.append(unpack(gathered, p, width))
        spreads.append(
            jnp.concatenate([weights[pl.ds(home[s], 1), :] for s in order], axis=1)
        )
        blocks.append(
            jnp.concatenate(
                [snap[:, pl.ds(pl.multiple_of(s * width, width), width)] for s in order], axis=1
            )
        )
    turns = rotations(grams, spreads)
    places = [[(send, 0), (keep, 0)], [(keep, 1), (send, 1)]]
    for p in range(2):
        q = split(turns[p])
        result = dot3(split(blocks[p]), q, 1, 0)
        moved = split(dot3(split(grams[p]), q, 1, 0))
        for h in range(2):
            ref, at = places[p][h]
            cut = slice(h * width, (h + 1) * width)
            own = dot3([x[:, cut] for x in q], [x[:, cut] for x in moved], 0, 0)
            ref[at, :rows, :] = result[:, cut]
            ref[at, rows : rows + width, :] = own
            ref[at, rows + width :, :] = jnp.broadcast_to(spreads[p][:, cut], (tile, width))


def gather_slots(keep, received, held):
    held[0] = received[0]
    held[1] = keep[0]
    held[2] = keep[1]
    held[3] = received[1]


def cross_kernel(plan, keep, received, out, held, *, rows, width):
    gather_slots(keep, received, held)
    n, chunk = out.shape[0], out.shape[1]
    crosses = []
    for p in range(2):
        a, b = [split(held[plan[1, 0, 2 * p + h], :rows, :]) for h in range(2)]
        crosses.append(dot3(a, b, 0, 0))
    for c in range(n):
        start = c * chunk
        if start < 2 * width:
            out[c] = crosses[start // width][start % width : start % width + chunk]
        else:
            out[c] = jnp.zeros((chunk, width), f32)


def second_kernel(plan, keep, received, gathered, send, kept, held, *, rows, width):
    gather_slots(keep, received, held)
    chunk = gathered.shape[1]
    per = width // chunk
    grams, spreads, blocks = [], [], []
    for p in range(2):
        order = [plan[1, 0, 2 * p + h] for h in range(2)]
        cross = jnp.concatenate([gathered[p * per + c] for c in range(per)], axis=0)
        own = [held[s, rows : rows + width, :] for s in order]
        grams.append(whole(own[0], cross, own[1]))
        spreads.append(
            jnp.concatenate([held[s, rows + width : rows + width + 1, :] for s in order], axis=1)
        )
        blocks.append(jnp.concatenate([held[s, :rows, :] for s in order], axis=1))
    turns = rotations(grams, spreads)
    places = [[(send, 0), (kept, 0)], [(kept, 1), (send, 1)]]
    for p in range(2):
        q = split(turns[p])
        result = dot3(split(blocks[p]), q, 1, 0)
        moved = dot3(split(grams[p]), q, 1, 0)
        squares = jnp.sum(turns[p] * moved, axis=0, keepdims=True)
        norms = jnp.sqrt(squares)
        for h in range(2):
            ref, at = places[p][h]
            cut = slice(h * width, (h + 1) * width)
            ref[at, :rows, :] = result[:, cut]
            ref[at, rows:, :] = jnp.broadcast_to(norms[:, cut], (tile, width))


def last_kernel(kept, received, final, norms):
    rows = final.shape[0]
    width = kept.shape[2]
    order = [(received, 0), (kept, 0), (kept, 1), (received, 1)]
    for s, (ref, at) in enumerate(order):
        final[:, s * width : (s + 1) * width] = ref[at, :rows, :]
        norms[s : s + 1, :] = ref[at, rows : rows + 1, :]


def near(x):
    return pltpu.with_memory_space_constraint(x, pltpu.VMEM)


def far(x):
    return pltpu.with_memory_space_constraint(x, pltpu.HBM)


def call(kernel, outs, specs, scratch=(), **static):
    def run(*refs):
        kernel(*refs, **static)

    run.__name__ = kernel.__name__
    return pl.pallas_call(
        run,
        out_shape=outs,
        in_specs=specs,
        out_specs=jax.tree.map(lambda _: VMEM, outs),
        scratch_shapes=scratch,
        compiler_params=pltpu.CompilerParams(vmem_limit_bytes=grant),
        name=kernel.__name__,
    )


def shape(*dims):
    return pltpu.VMEM(dims, f32)


def exchange(send):
    count = lax.axis_size("pair")
    ahead = [((i - 1) % count, i) for i in range(count)]
    behind = [((i + 1) % count, i) for i in range(count)]
    if sorted(ahead) == sorted(behind):
        return near(lax.ppermute(send, "pair", ahead))
    return jnp.stack(
        [lax.ppermute(send[0], "pair", ahead), lax.ppermute(send[1], "pair", behind)]
    )


def total(parts):
    mine = lax.all_to_all(parts, "row", 0, 0, tiled=True)
    summed = call(sum_kernel, shape(*parts.shape), [VMEM])(near(mine))
    return near(lax.all_to_all(summed, "row", 0, 0, tiled=True))


def body(snapshot, weights, block_home, plan):
    rows = snapshot.shape[0]
    width = weights.shape[1]
    n = lax.axis_size("row")
    packed = call(
        pack_kernel, shape(n, sizes(n, 4 * width) + tile, width), [SMEM, VMEM], width=width
    )(far(plan), far(snapshot))
    gathered = total(packed)
    tall = rows + width + tile
    send, keep = call(
        first_kernel,
        [shape(2, tall, width), shape(2, tall, width)],
        [SMEM, SMEM, VMEM, VMEM, VMEM],
        width=width,
    )(plan, block_home, weights, snapshot, gathered)
    received = exchange(send)
    scratch = [pltpu.VMEM((4, tall, width), f32)]
    cross = call(
        cross_kernel,
        shape(n, sizes(n, 2 * width), width),
        [SMEM, VMEM, VMEM],
        scratch,
        rows=rows,
        width=width,
    )(plan, keep, received)
    gathered = total(cross)
    send, kept = call(
        second_kernel,
        [shape(2, rows + tile, width), shape(2, rows + tile, width)],
        [SMEM, VMEM, VMEM, VMEM],
        scratch,
        rows=rows,
        width=width,
    )(plan, keep, received, gathered)
    final, norms = call(
        last_kernel,
        [jax.ShapeDtypeStruct((rows, 4 * width), f32), jax.ShapeDtypeStruct((4, width), f32)],
        [VMEM, VMEM],
    )(kept, exchange(send))
    return final, norms.reshape(4 * width)


def solution(mesh):
    in_specs = (P("row", "pair"), P(), P("pair"), P(None, "pair", None))
    out_specs = (P("row", "pair"), P("pair"))
    return jax.shard_map(body, mesh=mesh, in_specs=in_specs, out_specs=out_specs, check_vma=False)
```

```python
import jax
import jax.numpy as jnp
from jax import lax
from jax.experimental import pallas as pl
from jax.experimental.pallas import tpu as pltpu
from jax.sharding import PartitionSpec as P

epsilon = 1e-06
step_size = 4.0
newton_turns = 5
light_turn = 3
tile = 8
grant = 16 * 1024 * 1024
f32 = jnp.float32
bf16 = jnp.bfloat16

VMEM = pl.BlockSpec(memory_space=pltpu.VMEM)
SMEM = pl.BlockSpec(memory_space=pltpu.SMEM)
ANY = pl.BlockSpec(memory_space=pl.ANY)


def split(x):
    high = x.astype(bf16)
    return high, (x - high.astype(f32)).astype(bf16)


def dot(a, b, da, db):
    return lax.dot_general(a, b, (((da,), (db,)), ((), ())), preferred_element_type=f32)


def dot3(a, b, da, db):
    return dot(a[0], b[0], da, db) + (dot(a[0], b[1], da, db) + dot(a[1], b[0], da, db))


def iotas(n):
    return (
        lax.broadcasted_iota(jnp.int32, (n, n), 0),
        lax.broadcasted_iota(jnp.int32, (n, n), 1),
    )


def column(row):
    n = row.shape[1]
    return jnp.transpose(jnp.broadcast_to(row, (n, n)))


def start_rotation(gram, row_weight):
    n = gram.shape[0]
    i, j = iotas(n)
    same = i == j
    held = jnp.where(same, gram, 0.0)
    inv_row = lax.rsqrt(jnp.sum(held, axis=0, keepdims=True) + epsilon)
    inv_col = lax.rsqrt(jnp.sum(held, axis=1, keepdims=True) + epsilon)
    corr = gram * inv_col * inv_row
    skew = step_size * corr * (column(row_weight) - row_weight)
    bound = 1.0 + jnp.max(jnp.sum(jnp.abs(skew), axis=0, keepdims=True), axis=1, keepdims=True)
    return jnp.where(same, 1.0, 0.0) + skew * (1.0 / bound)


def rotations(grams, row_weights):
    n = grams[0].shape[0]
    i, j = iotas(n)
    same = i == j
    diag15 = jnp.where(same, 1.5, 0.0)
    diag05 = jnp.where(same, 0.5, 0.0)
    current = [start_rotation(g, w) for g, w in zip(grams, row_weights)]
    for turn in range(newton_turns):
        parts = [split(x) for x in current]
        inner = [dot3(p, p, 1, 1) for p in parts]
        if turn < light_turn:
            turns = [split(diag15 - 0.5 * y) for y in inner]
            current = [dot3(p, t, 1, 0) for p, t in zip(parts, turns)]
        else:
            fixes = [(diag05 - 0.5 * y).astype(bf16) for y in inner]
            current = [x + dot(p[0], e, 1, 0) for x, p, e in zip(current, parts, fixes)]
    return current


def sizes(n, rows):
    return max(tile, rows // n)


def pack_kernel(plan, snap, out, *, width):
    n, chunk = out.shape[0], out.shape[1] - tile
    i, j = iotas(width)
    held = []
    diags = []
    for p in range(2):
        ab = [
            snap[:, pl.ds(pl.multiple_of(plan[0, 0, 2 * p + h] * width, width), width)]
            for h in range(2)
        ]
        parts = split(jnp.concatenate(ab, axis=1))
        gram = dot3(parts, parts, 0, 0)
        upper = gram[:width, :width]
        lower = gram[width:, width:]
        held.append(gram[:width, width:])
        held.append(jnp.where(i <= j, upper, lower))
        diags.append(jnp.sum(jnp.where(i == j, lower, 0.0), axis=0, keepdims=True))
    extra = jnp.concatenate(diags + [jnp.zeros((tile - 2, width), f32)], axis=0)
    for c in range(n):
        start = c * chunk
        out[c, :chunk, :] = held[start // width][start % width : start % width + chunk]
        out[c, chunk:, :] = extra if c == 0 else jnp.zeros((tile, width), f32)


def sum_kernel(parts, out):
    n = parts.shape[0]
    values = [parts[c] for c in range(n)]
    while len(values) > 1:
        values = [a + b for a, b in zip(values[0::2], values[1::2])] + (
            [values[-1]] if len(values) % 2 else []
        )
    for c in range(n):
        out[c] = values[0]


def unpack(gathered, p, width):
    chunk = gathered.shape[1] - tile
    rows = []
    per = width // chunk
    for q in range(2):
        first = (2 * p + q) * per
        rows.append(jnp.concatenate([gathered[first + c, :chunk, :] for c in range(per)], axis=0))
    cross, both = rows
    i, j = iotas(width)
    flipped = jnp.transpose(both)
    diag_b = gathered[0, chunk + p : chunk + p + 1, :]
    upper = jnp.where(i <= j, both, flipped)
    lower = jnp.where(i > j, both, jnp.where(i == j, diag_b, flipped))
    return whole(upper, cross, lower)


def whole(upper, cross, lower):
    return jnp.concatenate(
        [
            jnp.concatenate([upper, cross], axis=1),
            jnp.concatenate([jnp.transpose(cross), lower], axis=1),
        ],
        axis=0,
    )


def pair_of(snap, plan, p, width):
    return jnp.concatenate(
        [
            snap[:, pl.ds(pl.multiple_of(plan[0, 0, 2 * p + h] * width, width), width)]
            for h in range(2)
        ],
        axis=1,
    )


def half(x, h):
    width = x.shape[1] // 2
    return x[:, h * width : (h + 1) * width]


def first_kernel(plan, home, weights, snap, gathered, send, turned, spread, *, width):
    rows = snap.shape[0]
    grams, spreads = [], []
    for p in range(2):
        grams.append(unpack(gathered, p, width))
        spreads.append(
            jnp.concatenate(
                [weights[pl.ds(home[plan[0, 0, 2 * p + h]], 1), :] for h in range(2)], axis=1
            )
        )
    turns = rotations(grams, spreads)
    for p in range(2):
        q = half(turns[p], p)
        send[p, :rows, :] = dot3(split(pair_of(snap, plan, p, width)), split(q), 1, 0)
        send[p, rows:, :] = jnp.broadcast_to(half(spreads[p], p), (tile, width))
        spread[p] = jnp.broadcast_to(half(spreads[p], 1 - p), (tile, width))
        turned[p] = turns[p]


def stay_kernel(plan, snap, turned, keep, *, width):
    for p in range(2):
        q = half(turned[p], 1 - p)
        keep[p] = dot3(split(pair_of(snap, plan, p, width)), split(q), 1, 0)


def carry_kernel(gathered, turned, send, keep, *, width):
    for p in range(2):
        q = split(turned[p])
        moved = split(dot3(split(unpack(gathered, p, width)), q, 1, 0))
        for h in range(2):
            own = dot3([half(x, h) for x in q], [half(x, h) for x in moved], 0, 0)
            (send if h == p else keep)[p] = own


def slot_value(s, received, keep, cut):
    values = [received[0, cut, :], keep[0, cut, :], keep[1, cut, :], received[1, cut, :]]
    return jnp.where(s < 2, jnp.where(s == 0, *values[:2]), jnp.where(s == 2, *values[2:]))


def cross_kernel(plan, keep, received, out, *, rows, width):
    n, chunk = out.shape[0], out.shape[1]
    cut = slice(0, rows)
    crosses = []
    for p in range(2):
        a, b = [split(slot_value(plan[1, 0, 2 * p + h], received, keep, cut)) for h in range(2)]
        crosses.append(dot3(a, b, 0, 0))
    for c in range(n):
        start = c * chunk
        if start < 2 * width:
            out[c] = crosses[start // width][start % width : start % width + chunk]
        else:
            out[c] = jnp.zeros((chunk, width), f32)


def second_kernel(
    plan, keep, received, spread, own_keep, own_received, gathered, send, turned, norms, *, rows
):
    width = keep.shape[2]
    chunk = gathered.shape[1]
    per = width // chunk
    every = slice(0, width)
    grams, spreads = [], []
    for p in range(2):
        order = [plan[1, 0, 2 * p + h] for h in range(2)]
        cross = jnp.concatenate([gathered[p * per + c] for c in range(per)], axis=0)
        own = [slot_value(s, own_received, own_keep, every) for s in order]
        grams.append(whole(own[0], cross, own[1]))
        wide = [received[0, rows:, :], spread[0], spread[1], received[1, rows:, :]]
        spreads.append(
            jnp.concatenate(
                [
                    jnp.where(
                        s < 2, jnp.where(s == 0, *wide[:2]), jnp.where(s == 2, *wide[2:])
                    )[:1]
                    for s in order
                ],
                axis=1,
            )
        )
    turns = rotations(grams, spreads)
    for p in range(2):
        q = split(turns[p])
        block = pair_after(plan, keep, received, p, rows)
        send[p, :rows, :] = dot3(split(block), [half(x, p) for x in q], 1, 0)
        moved = dot3(split(grams[p]), q, 1, 0)
        squares = jnp.sum(turns[p] * moved, axis=0, keepdims=True)
        lengths = jnp.sqrt(squares)
        send[p, rows:, :] = jnp.broadcast_to(half(lengths, p), (tile, width))
        norms[p] = jnp.broadcast_to(half(lengths, 1 - p), (tile, width))
        turned[p] = half(turns[p], 1 - p)


def pair_after(plan, keep, received, p, rows):
    return jnp.concatenate(
        [
            slot_value(plan[1, 0, 2 * p + h], received, keep, slice(0, rows))
            for h in range(2)
        ],
        axis=1,
    )


def finish_kernel(plan, keep, received, turned, final, held, sems, *, rows):
    width = keep.shape[2]
    copies = []
    for p in range(2):
        block = pair_after(plan, keep, received, p, rows)
        held[p] = dot3(split(block), split(turned[p]), 1, 0)
        at = (1 + p) * width
        copy = pltpu.make_async_copy(held.at[p], final.at[:, at : at + width], sems.at[p])
        copy.start()
        copies.append(copy)
    for copy in copies:
        copy.wait()


def last_kernel(partly, norms_here, received, final, norms, sems):
    del partly
    rows = final.shape[0]
    width = received.shape[2]
    copies = []
    for p in range(2):
        at = 3 * p * width
        copy = pltpu.make_async_copy(
            received.at[p, :rows, :], final.at[:, at : at + width], sems.at[p]
        )
        copy.start()
        copies.append(copy)
    norms[0:1, :] = received[0, rows : rows + 1, :]
    norms[1:2, :] = norms_here[0, :1, :]
    norms[2:3, :] = norms_here[1, :1, :]
    norms[3:4, :] = received[1, rows : rows + 1, :]
    for copy in copies:
        copy.wait()


def near(x):
    return pltpu.with_memory_space_constraint(x, pltpu.VMEM)


def far(x):
    return pltpu.with_memory_space_constraint(x, pltpu.HBM)


def call(kernel, outs, specs, scratch=(), out_specs=None, aliases=None, **static):
    def run(*refs):
        kernel(*refs, **static)

    return pl.pallas_call(
        run,
        out_shape=outs,
        in_specs=specs,
        out_specs=jax.tree.map(lambda _: VMEM, outs) if out_specs is None else out_specs,
        scratch_shapes=scratch,
        input_output_aliases=aliases or {},
        compiler_params=pltpu.CompilerParams(vmem_limit_bytes=grant),
        name=kernel.__name__,
    )


def shape(*dims):
    return pltpu.VMEM(dims, f32)


def exchange(send):
    count = lax.axis_size("pair")
    ahead = [((i - 1) % count, i) for i in range(count)]
    behind = [((i + 1) % count, i) for i in range(count)]
    if sorted(ahead) == sorted(behind):
        return near(lax.ppermute(send, "pair", ahead))
    return jnp.stack(
        [lax.ppermute(send[0], "pair", ahead), lax.ppermute(send[1], "pair", behind)]
    )


def total(parts):
    mine = lax.all_to_all(parts, "row", 0, 0, tiled=True)
    summed = call(sum_kernel, shape(*parts.shape), [VMEM])(near(mine))
    return near(lax.all_to_all(summed, "row", 0, 0, tiled=True))


def body(snapshot, weights, block_home, plan):
    rows = snapshot.shape[0]
    width = weights.shape[1]
    n = lax.axis_size("row")
    packed = call(
        pack_kernel, shape(n, sizes(n, 4 * width) + tile, width), [SMEM, VMEM], width=width
    )(far(plan), far(snapshot))
    gathered = total(packed)
    send, turned, spread = call(
        first_kernel,
        [shape(2, rows + tile, width), shape(2, 2 * width, 2 * width), shape(2, tile, width)],
        [SMEM, SMEM, VMEM, VMEM, VMEM],
        width=width,
    )(plan, block_home, weights, snapshot, gathered)
    received = exchange(send)
    keep = call(stay_kernel, shape(2, rows, width), [SMEM, VMEM, VMEM], width=width)(
        plan, snapshot, turned
    )
    cross = call(
        cross_kernel,
        shape(n, sizes(n, 2 * width), width),
        [SMEM, VMEM, VMEM],
        rows=rows,
        width=width,
    )(plan, keep, received)
    own_send, own_keep = call(
        carry_kernel,
        [shape(2, width, width), shape(2, width, width)],
        [VMEM, VMEM],
        width=width,
    )(gathered, turned)
    own_received = exchange(own_send)
    gathered = total(cross)
    send, turned, norms = call(
        second_kernel,
        [shape(2, rows + tile, width), shape(2, 2 * width, width), shape(2, tile, width)],
        [SMEM] + [VMEM] * 6,
        rows=rows,
    )(plan, keep, received, spread, own_keep, own_received, gathered)
    arrived = exchange(send)
    final_shape = jax.ShapeDtypeStruct((rows, 4 * width), f32)
    partly = call(
        finish_kernel,
        final_shape,
        [SMEM, VMEM, VMEM, VMEM],
        [pltpu.VMEM((2, rows, width), f32), pltpu.SemaphoreType.DMA((2,))],
        ANY,
        rows=rows,
    )(plan, keep, received, turned)
    final, norms = call(
        last_kernel,
        [final_shape, jax.ShapeDtypeStruct((4, width), f32)],
        [ANY, VMEM, VMEM],
        [pltpu.SemaphoreType.DMA((2,))],
        [ANY, VMEM],
        {0: 0},
    )(partly, norms, arrived)
    return final, norms.reshape(4 * width)


def solution(mesh):
    in_specs = (P("row", "pair"), P(), P("pair"), P(None, "pair", None))
    out_specs = (P("row", "pair"), P("pair"))
    return jax.shard_map(body, mesh=mesh, in_specs=in_specs, out_specs=out_specs, check_vma=False)
```

```python
import jax
import jax.numpy as jnp
from jax import lax
from jax.experimental import pallas as pl
from jax.experimental.pallas import tpu as pltpu
from jax.sharding import PartitionSpec as P

epsilon = 1e-06
step_size = 4.0
newton_turns = 5
light_turn = 3
tile = 8
grant = 16 * 1024 * 1024
f32 = jnp.float32
bf16 = jnp.bfloat16

VMEM = pl.BlockSpec(memory_space=pltpu.VMEM)
SMEM = pl.BlockSpec(memory_space=pltpu.SMEM)


def split(x):
    high = x.astype(bf16)
    return high, (x - high.astype(f32)).astype(bf16)


def dot(a, b, da, db):
    return lax.dot_general(a, b, (((da,), (db,)), ((), ())), preferred_element_type=f32)


def dot3(a, b, da, db):
    return dot(a[0], b[0], da, db) + (dot(a[0], b[1], da, db) + dot(a[1], b[0], da, db))


def iotas(n):
    return (
        lax.broadcasted_iota(jnp.int32, (n, n), 0),
        lax.broadcasted_iota(jnp.int32, (n, n), 1),
    )


def column(row):
    n = row.shape[1]
    return jnp.transpose(jnp.broadcast_to(row, (n, n)))


def start_rotation(gram, row_weight):
    n = gram.shape[0]
    i, j = iotas(n)
    same = i == j
    held = jnp.where(same, gram, 0.0)
    inv_row = lax.rsqrt(jnp.sum(held, axis=0, keepdims=True) + epsilon)
    inv_col = lax.rsqrt(jnp.sum(held, axis=1, keepdims=True) + epsilon)
    corr = gram * inv_col * inv_row
    skew = step_size * corr * (column(row_weight) - row_weight)
    bound = 1.0 + jnp.max(jnp.sum(jnp.abs(skew), axis=0, keepdims=True), axis=1, keepdims=True)
    return jnp.where(same, 1.0, 0.0) + skew * (1.0 / bound)


def rotations(grams, row_weights):
    n = grams[0].shape[0]
    i, j = iotas(n)
    same = i == j
    diag15 = jnp.where(same, 1.5, 0.0)
    diag05 = jnp.where(same, 0.5, 0.0)
    current = [start_rotation(g, w) for g, w in zip(grams, row_weights)]
    for turn in range(newton_turns):
        parts = [split(x) for x in current]
        inner = [dot3(p, p, 1, 1) for p in parts]
        if turn < light_turn:
            turns = [split(diag15 - 0.5 * y) for y in inner]
            current = [dot3(p, t, 1, 0) for p, t in zip(parts, turns)]
        else:
            fixes = [(diag05 - 0.5 * y).astype(bf16) for y in inner]
            current = [x + dot(p[0], e, 1, 0) for x, p, e in zip(current, parts, fixes)]
    return current


def sizes(n, rows):
    return max(tile, rows // n)


def pack_kernel(plan, snap, out, *, width):
    n, chunk = out.shape[0], out.shape[1] - tile
    i, j = iotas(width)
    held = []
    diags = []
    for p in range(2):
        ab = [
            snap[:, pl.ds(pl.multiple_of(plan[0, 0, 2 * p + h] * width, width), width)]
            for h in range(2)
        ]
        parts = split(jnp.concatenate(ab, axis=1))
        gram = dot3(parts, parts, 0, 0)
        upper = gram[:width, :width]
        lower = gram[width:, width:]
        held.append(gram[:width, width:])
        held.append(jnp.where(i <= j, upper, lower))
        diags.append(jnp.sum(jnp.where(i == j, lower, 0.0), axis=0, keepdims=True))
    extra = jnp.concatenate(diags + [jnp.zeros((tile - 2, width), f32)], axis=0)
    for c in range(n):
        start = c * chunk
        out[c, :chunk, :] = held[start // width][start % width : start % width + chunk]
        out[c, chunk:, :] = extra if c == 0 else jnp.zeros((tile, width), f32)


def added(values):
    while len(values) > 1:
        values = [a + b for a, b in zip(values[0::2], values[1::2])] + (
            [values[-1]] if len(values) % 2 else []
        )
    return values[0]


def sum_kernel(parts, out):
    n = parts.shape[0]
    value = added([parts[c] for c in range(n)])
    for c in range(n):
        out[c] = value


def half_sum_kernel(parts, out):
    out[...] = added([parts[c] for c in range(parts.shape[0])])


def join_kernel(here, there, out):
    value = here[...] + there[...]
    for c in range(out.shape[0]):
        out[c] = value


def unpack(gathered, p, width):
    chunk = gathered.shape[1] - tile
    rows = []
    per = width // chunk
    for q in range(2):
        first = (2 * p + q) * per
        rows.append(jnp.concatenate([gathered[first + c, :chunk, :] for c in range(per)], axis=0))
    cross, both = rows
    i, j = iotas(width)
    flipped = jnp.transpose(both)
    diag_b = gathered[0, chunk + p : chunk + p + 1, :]
    upper = jnp.where(i <= j, both, flipped)
    lower = jnp.where(i > j, both, jnp.where(i == j, diag_b, flipped))
    return whole(upper, cross, lower)


def whole(upper, cross, lower):
    return jnp.concatenate(
        [
            jnp.concatenate([upper, cross], axis=1),
            jnp.concatenate([jnp.transpose(cross), lower], axis=1),
        ],
        axis=0,
    )


def pair_of(snap, plan, p, width):
    return jnp.concatenate(
        [
            snap[:, pl.ds(pl.multiple_of(plan[0, 0, 2 * p + h] * width, width), width)]
            for h in range(2)
        ],
        axis=1,
    )


def half(x, h):
    width = x.shape[1] // 2
    return x[:, h * width : (h + 1) * width]


def own_gram(gram, q):
    return dot3(q, split(dot3(split(gram), q, 1, 0)), 0, 0)


def first_kernel(plan, home, weights, snap, gathered, send, turned, spread, *, width):
    rows = snap.shape[0]
    grams, spreads = [], []
    for p in range(2):
        grams.append(unpack(gathered, p, width))
        spreads.append(
            jnp.concatenate(
                [weights[pl.ds(home[plan[0, 0, 2 * p + h]], 1), :] for h in range(2)], axis=1
            )
        )
    turns = rotations(grams, spreads)
    for p in range(2):
        q = split(half(turns[p], p))
        send[p, :rows, :] = dot3(split(pair_of(snap, plan, p, width)), q, 1, 0)
        send[p, rows : rows + width, :] = own_gram(grams[p], q)
        send[p, rows + width :, :] = jnp.broadcast_to(half(spreads[p], p), (tile, width))
        spread[p] = jnp.broadcast_to(half(spreads[p], 1 - p), (tile, width))
        turned[p] = half(turns[p], 1 - p)


def stay_kernel(plan, snap, gathered, turned, spread, keep, *, width):
    rows = snap.shape[0]
    for p in range(2):
        q = split(turned[p])
        keep[p, :rows, :] = dot3(split(pair_of(snap, plan, p, width)), q, 1, 0)
        keep[p, rows : rows + width, :] = own_gram(unpack(gathered, p, width), q)
        keep[p, rows + width :, :] = spread[p]


def slot_value(s, received, keep, cut):
    values = [received[0, cut, :], keep[0, cut, :], keep[1, cut, :], received[1, cut, :]]
    return jnp.where(s < 2, jnp.where(s == 0, *values[:2]), jnp.where(s == 2, *values[2:]))


def cross_kernel(plan, keep, received, out, high, low, *, rows, width):
    n, chunk = out.shape[0], out.shape[1]
    crosses = []
    for p in range(2):
        blocks = []
        for h in range(2):
            at = slice(h * width, (h + 1) * width)
            block = split(slot_value(plan[1, 0, 2 * p + h], received, keep, slice(0, rows)))
            high[p, :, at] = block[0]
            low[p, :, at] = block[1]
            blocks.append(block)
        crosses.append(dot3(*blocks, 0, 0))
    for c in range(n):
        start = c * chunk
        if start < 2 * width:
            out[c] = crosses[start // width][start % width : start % width + chunk]
        else:
            out[c] = jnp.zeros((chunk, width), f32)


def second_kernel(plan, keep, received, high, low, gathered, send, turned, norms, *, rows, width):
    chunk = gathered.shape[1]
    per = width // chunk
    grams, spreads = [], []
    for p in range(2):
        order = [plan[1, 0, 2 * p + h] for h in range(2)]
        cross = jnp.concatenate([gathered[p * per + c] for c in range(per)], axis=0)
        own = [slot_value(s, received, keep, slice(rows, rows + width)) for s in order]
        grams.append(whole(own[0], cross, own[1]))
        wide = [
            slot_value(s, received, keep, slice(rows + width, rows + width + 1)) for s in order
        ]
        spreads.append(jnp.concatenate(wide, axis=1))
    turns = rotations(grams, spreads)
    for p in range(2):
        q = split(turns[p])
        send[p, :rows, :] = dot3((high[p], low[p]), [half(x, p) for x in q], 1, 0)
        moved = dot3(split(grams[p]), q, 1, 0)
        squares = jnp.sum(turns[p] * moved, axis=0, keepdims=True)
        lengths = jnp.sqrt(squares)
        send[p, rows:, :] = jnp.broadcast_to(half(lengths, p), (tile, width))
        norms[p] = jnp.broadcast_to(half(lengths, 1 - p), (tile, width))
        turned[p] = half(turns[p], 1 - p)


def finish_kernel(high, low, turned, kept):
    for p in range(2):
        kept[p] = dot3((high[p], low[p]), split(turned[p]), 1, 0)


def last_kernel(kept, norms_here, received, final, norms):
    rows, width = kept.shape[1], kept.shape[2]
    order = [received[0, :rows, :], kept[0], kept[1], received[1, :rows, :]]
    lengths = [received[0, rows:, :], norms_here[0], norms_here[1], received[1, rows:, :]]
    for s in range(4):
        final[:, s * width : (s + 1) * width] = order[s]
        norms[s : s + 1, :] = lengths[s][:1]


def near(x):
    return pltpu.with_memory_space_constraint(x, pltpu.VMEM)


def far(x):
    return pltpu.with_memory_space_constraint(x, pltpu.HBM)


def call(kernel, outs, specs, **static):
    def run(*refs):
        kernel(*refs, **static)

    return pl.pallas_call(
        run,
        out_shape=outs,
        in_specs=specs,
        out_specs=jax.tree.map(lambda _: VMEM, outs),
        compiler_params=pltpu.CompilerParams(vmem_limit_bytes=grant),
        name=kernel.__name__,
    )


def shape(*dims):
    return pltpu.VMEM(dims, f32)


def exchange(send):
    count = lax.axis_size("pair")
    ahead = [((i - 1) % count, i) for i in range(count)]
    behind = [((i + 1) % count, i) for i in range(count)]
    if sorted(ahead) == sorted(behind):
        return near(lax.ppermute(send, "pair", ahead))
    return jnp.stack(
        [lax.ppermute(send[0], "pair", ahead), lax.ppermute(send[1], "pair", behind)]
    )


def swap(parts, groups=None):
    return near(
        lax.all_to_all(parts, "row", 0, 0, tiled=True, axis_index_groups=groups)
    )


def total(parts):
    mine = swap(parts)
    return swap(call(sum_kernel, shape(*parts.shape), [VMEM])(mine))


def halved_total(parts):
    n = lax.axis_size("row")
    reach = n // 2
    groups = [list(range(reach)), list(range(reach, n))]
    mine = swap(parts, groups)
    here = call(half_sum_kernel, shape(*parts.shape[1:]), [VMEM])(mine)
    there = near(lax.ppermute(here, "row", [(i, (i + reach) % n) for i in range(n)]))
    both = call(join_kernel, shape(*parts.shape), [VMEM, VMEM])(here, there)
    return swap(both, groups)


def body(snapshot, weights, block_home, plan):
    rows = snapshot.shape[0]
    width = weights.shape[1]
    n = lax.axis_size("row")
    reach = n // 2
    packed = call(
        pack_kernel, shape(reach, sizes(reach, 4 * width) + tile, width), [SMEM, VMEM], width=width
    )(far(plan), far(snapshot))
    gathered = halved_total(packed)
    tall = rows + width + tile
    send, turned, spread = call(
        first_kernel,
        [shape(2, tall, width), shape(2, 2 * width, width), shape(2, tile, width)],
        [SMEM, SMEM, VMEM, VMEM, VMEM],
        width=width,
    )(plan, block_home, weights, snapshot, gathered)
    received = exchange(send)
    keep = call(
        stay_kernel, shape(2, tall, width), [SMEM, VMEM, VMEM, VMEM, VMEM], width=width
    )(plan, snapshot, gathered, turned, spread)
    wide = pltpu.VMEM((2, rows, 2 * width), bf16)
    cross, high, low = call(
        cross_kernel,
        [shape(n, sizes(n, 2 * width), width), wide, wide],
        [SMEM, VMEM, VMEM],
        rows=rows,
        width=width,
    )(plan, keep, received)
    gathered = total(cross)
    send, turned, norms = call(
        second_kernel,
        [shape(2, rows + tile, width), shape(2, 2 * width, width), shape(2, tile, width)],
        [SMEM] + [VMEM] * 5,
        rows=rows,
        width=width,
    )(plan, keep, received, high, low, gathered)
    arrived = exchange(send)
    kept = call(finish_kernel, shape(2, rows, width), [VMEM, VMEM, VMEM])(high, low, turned)
    final, norms = call(
        last_kernel,
        [jax.ShapeDtypeStruct((rows, 4 * width), f32), jax.ShapeDtypeStruct((4, width), f32)],
        [VMEM, VMEM, VMEM],
    )(kept, norms, arrived)
    return final, norms.reshape(4 * width)


def solution(mesh):
    in_specs = (P("row", "pair"), P(), P("pair"), P(None, "pair", None))
    out_specs = (P("row", "pair"), P("pair"))
    return jax.shard_map(body, mesh=mesh, in_specs=in_specs, out_specs=out_specs, check_vma=False)
```

```python
import jax
import jax.numpy as jnp
from jax import lax
from jax.experimental import pallas as pl
from jax.experimental.pallas import tpu as pltpu
from jax.sharding import PartitionSpec as P

epsilon = 1e-06
step_size = 4.0
newton_turns = 5
light_turn = 3
tile = 8
grant = 16 * 1024 * 1024
f32 = jnp.float32
bf16 = jnp.bfloat16

VMEM = pl.BlockSpec(memory_space=pltpu.VMEM)
SMEM = pl.BlockSpec(memory_space=pltpu.SMEM)


def split(x):
    high = x.astype(bf16)
    return high, (x - high.astype(f32)).astype(bf16)


def dot(a, b, da, db):
    return lax.dot_general(a, b, (((da,), (db,)), ((), ())), preferred_element_type=f32)


def dot3(a, b, da, db):
    return dot(a[0], b[0], da, db) + (dot(a[0], b[1], da, db) + dot(a[1], b[0], da, db))


def iotas(n):
    return (
        lax.broadcasted_iota(jnp.int32, (n, n), 0),
        lax.broadcasted_iota(jnp.int32, (n, n), 1),
    )


def column(row):
    n = row.shape[1]
    return jnp.transpose(jnp.broadcast_to(row, (n, n)))


def start_rotation(gram, row_weight):
    n = gram.shape[0]
    i, j = iotas(n)
    same = i == j
    held = jnp.where(same, gram, 0.0)
    inv_row = lax.rsqrt(jnp.sum(held, axis=0, keepdims=True) + epsilon)
    inv_col = lax.rsqrt(jnp.sum(held, axis=1, keepdims=True) + epsilon)
    corr = gram * inv_col * inv_row
    skew = step_size * corr * (column(row_weight) - row_weight)
    bound = 1.0 + jnp.max(jnp.sum(jnp.abs(skew), axis=0, keepdims=True), axis=1, keepdims=True)
    return jnp.where(same, 1.0, 0.0) + skew * (1.0 / bound)


def rotations(grams, row_weights, fillers=()):
    n = grams[0].shape[0]
    i, j = iotas(n)
    same = i == j
    diag15 = jnp.where(same, 1.5, 0.0)
    diag05 = jnp.where(same, 0.5, 0.0)
    current = [start_rotation(g, w) for g, w in zip(grams, row_weights)]
    for turn in range(newton_turns):
        parts = [split(x) for x in current]
        inner = [dot3(p, p, 1, 1) for p in parts]
        if turn < len(fillers):
            fillers[turn]()
        if turn < light_turn:
            turns = [split(diag15 - 0.5 * y) for y in inner]
            current = [dot3(p, t, 1, 0) for p, t in zip(parts, turns)]
        else:
            fixes = [(diag05 - 0.5 * y).astype(bf16) for y in inner]
            current = [x + dot(p[0], e, 1, 0) for x, p, e in zip(current, parts, fixes)]
    return current


def sizes(n, rows):
    return max(tile, rows // n)


def chunk_rows(reach, width):
    return sizes(reach, 4 * width), sizes(reach, 8 * width), tile


def pair_of(snap, plan, p, width):
    return jnp.concatenate(
        [
            snap[:, pl.ds(pl.multiple_of(plan[0, 0, 2 * p + h] * width, width), width)]
            for h in range(2)
        ],
        axis=1,
    )


def pack_kernel(plan, snap, out, high, low, *, width):
    reach = out.shape[0]
    main, raw, _ = chunk_rows(reach, width)
    i, j = iotas(width)
    held = []
    diags = []
    for p in range(2):
        parts = split(pair_of(snap, plan, p, width))
        high[1 + p] = parts[0]
        low[1 + p] = parts[1]
        gram = dot3(parts, parts, 0, 0)
        upper = gram[:width, :width]
        lower = gram[width:, width:]
        held.append(gram[:width, width:])
        held.append(jnp.where(i <= j, upper, lower))
        diags.append(jnp.sum(jnp.where(i == j, lower, 0.0), axis=0, keepdims=True))
    extra = jnp.concatenate(diags + [jnp.zeros((tile - 2, width), f32)], axis=0)
    for c in range(reach):
        start = c * main
        out[c, :main, :] = held[start // width][start % width : start % width + main]
        out[c, main + raw :, :] = extra if c == 0 else jnp.zeros((tile, width), f32)


def raw_kernel(
    plan, plan_ahead, plan_behind, ahead, behind, packed, own_high, own_low, out, high, low, *, width
):
    del packed, own_high, own_low
    for s, snap, order, p in [(0, ahead, plan_ahead, 0), (3, behind, plan_behind, 1)]:
        parts = split(pair_of(snap, order, p, width))
        high[s] = parts[0]
        low[s] = parts[1]
    reach = out.shape[0]
    main, raw, _ = chunk_rows(reach, width)
    crosses = []
    for r in range(2):
        a, b = [plan[1, 0, 2 * r + h] for h in range(2)]
        crosses.append(dot3((high[b], low[b]), (high[a], low[a]), 0, 0))
    tall = 2 * width
    for c in range(reach):
        block, at = divmod(c * raw, tall)
        out[c, main : main + raw, :] = half(crosses[block // 2], block % 2)[at : at + raw]


def half(x, h):
    width = x.shape[1] // 2
    return x[:, h * width : (h + 1) * width]


def added(values):
    while len(values) > 1:
        values = [a + b for a, b in zip(values[0::2], values[1::2])] + (
            [values[-1]] if len(values) % 2 else []
        )
    return values[0]


def half_sum_kernel(parts, out):
    out[...] = added([parts[c] for c in range(parts.shape[0])])


def join_kernel(here, there, out):
    value = here[...] + there[...]
    for c in range(out.shape[0]):
        out[c] = value


def unpack(gathered, p, width):
    main, raw, _ = chunk_rows(gathered.shape[0], width)
    per = width // main
    cross, both = [
        jnp.concatenate(
            [gathered[(2 * p + q) * per + c, :main, :] for c in range(per)], axis=0
        )
        for q in range(2)
    ]
    i, j = iotas(width)
    flipped = jnp.transpose(both)
    diag_b = gathered[0, main + raw + p : main + raw + p + 1, :]
    upper = jnp.where(i <= j, both, flipped)
    lower = jnp.where(i > j, both, jnp.where(i == j, diag_b, flipped))
    return whole(upper, cross, jnp.transpose(cross), lower)


def unpack_raw(gathered, r, width):
    main, raw, _ = chunk_rows(gathered.shape[0], width)
    per = 2 * width // raw
    return jnp.concatenate(
        [
            jnp.concatenate(
                [
                    gathered[(2 * r + h) * per + c, main : main + raw, :]
                    for c in range(per)
                ],
                axis=0,
            )
            for h in range(2)
        ],
        axis=1,
    )


def whole(upper, cross, flipped, lower):
    return jnp.concatenate(
        [
            jnp.concatenate([upper, cross], axis=1),
            jnp.concatenate([flipped, lower], axis=1),
        ],
        axis=0,
    )


def own_gram(gram, q):
    return dot3(q, split(dot3(split(gram), q, 1, 0)), 0, 0)


def first_kernel(plan, home, weights, gathered, send, turned, spread, *, width):
    tall = 2 * width
    grams, spreads = [], []
    for p in range(2):
        grams.append(unpack(gathered, p, width))
        spreads.append(
            jnp.concatenate(
                [weights[pl.ds(home[plan[0, 0, 2 * p + h]], 1), :] for h in range(2)], axis=1
            )
        )
    turns = rotations(grams, spreads)
    for p in range(2):
        q = half(turns[p], p)
        send[p, :tall, :] = q
        send[p, tall : tall + width, :] = own_gram(grams[p], split(q))
        send[p, tall + width :, :] = jnp.broadcast_to(half(spreads[p], p), (tile, width))
        spread[p] = jnp.broadcast_to(half(spreads[p], 1 - p), (tile, width))
        turned[p] = half(turns[p], 1 - p)


def stay_kernel(gathered, turned, spread, keep, *, width):
    tall = 2 * width
    for p in range(2):
        q = turned[p]
        keep[p, :tall, :] = q
        keep[p, tall : tall + width, :] = own_gram(unpack(gathered, p, width), split(q))
        keep[p, tall + width :, :] = spread[p]


def slot_value(s, received, keep, cut):
    values = [received[0, cut, :], keep[0, cut, :], keep[1, cut, :], received[1, cut, :]]
    return jnp.where(s < 2, jnp.where(s == 0, *values[:2]), jnp.where(s == 2, *values[2:]))


def second_kernel(
    plan, keep, received, gathered, high, low, send, turned, norms, block_high, block_low, *, width
):
    tall = 2 * width
    rows = high.shape[1]
    grams, spreads, fillers = [], [], []

    def filler(r, h, s, q):
        def block():
            at = slice(h * width, (h + 1) * width)
            value = split(dot3((high[s], low[s]), q, 1, 0))
            block_high[r, :, at] = value[0]
            block_low[r, :, at] = value[1]

        return block

    for r in range(2):
        order = [plan[1, 0, 2 * r + h] for h in range(2)]
        first, second = [split(slot_value(s, received, keep, slice(0, tall))) for s in order]
        moved = dot3(split(unpack_raw(gathered, r, width)), first, 1, 0)
        flipped = dot3(second, split(moved), 0, 0)
        own = [slot_value(s, received, keep, slice(tall, tall + width)) for s in order]
        grams.append(whole(own[0], jnp.transpose(flipped), flipped, own[1]))
        wide = [
            slot_value(s, received, keep, slice(tall + width, tall + width + 1)) for s in order
        ]
        spreads.append(jnp.concatenate(wide, axis=1))
        fillers += [filler(r, h, s, q) for h, (s, q) in enumerate(zip(order, (first, second)))]
    turns = rotations(grams, spreads, fillers)
    for p in range(2):
        q = split(turns[p])
        send[p, :rows, :] = dot3(
            (block_high[p], block_low[p]), [half(x, p) for x in q], 1, 0
        )
        moved = dot3(split(grams[p]), q, 1, 0)
        squares = jnp.sum(turns[p] * moved, axis=0, keepdims=True)
        lengths = jnp.sqrt(squares)
        send[p, rows:, :] = jnp.broadcast_to(half(lengths, p), (tile, width))
        norms[p] = jnp.broadcast_to(half(lengths, 1 - p), (tile, width))
        turned[p] = half(turns[p], 1 - p)


def finish_kernel(high, low, turned, kept):
    for p in range(2):
        kept[p] = dot3((high[p], low[p]), split(turned[p]), 1, 0)


def last_kernel(kept, norms_here, received, final, norms):
    rows, width = kept.shape[1], kept.shape[2]
    order = [received[0, :rows, :], kept[0], kept[1], received[1, :rows, :]]
    lengths = [received[0, rows:, :], norms_here[0], norms_here[1], received[1, rows:, :]]
    for s in range(4):
        final[:, s * width : (s + 1) * width] = order[s]
        norms[s : s + 1, :] = lengths[s][:1]


def near(x):
    return pltpu.with_memory_space_constraint(x, pltpu.VMEM)


def far(x):
    return pltpu.with_memory_space_constraint(x, pltpu.HBM)


def call(kernel, outs, specs, aliases=None, **static):
    def run(*refs):
        kernel(*refs, **static)

    return pl.pallas_call(
        run,
        out_shape=outs,
        in_specs=specs,
        out_specs=jax.tree.map(lambda _: VMEM, outs),
        input_output_aliases=aliases or {},
        compiler_params=pltpu.CompilerParams(vmem_limit_bytes=grant),
        name=kernel.__name__,
    )


def shape(*dims):
    return pltpu.VMEM(dims, f32)


def routes():
    count = lax.axis_size("pair")
    ahead = [((i - 1) % count, i) for i in range(count)]
    behind = [((i + 1) % count, i) for i in range(count)]
    return ahead, behind, sorted(ahead) == sorted(behind)


def both_ways(x):
    ahead, behind, alike = routes()
    first = lax.ppermute(x, "pair", ahead)
    return first, first if alike else lax.ppermute(x, "pair", behind)


def exchange(send):
    ahead, behind, alike = routes()
    if alike:
        return near(lax.ppermute(send, "pair", ahead))
    return jnp.stack(
        [lax.ppermute(send[0], "pair", ahead), lax.ppermute(send[1], "pair", behind)]
    )


def swap(parts, groups=None):
    return near(
        lax.all_to_all(parts, "row", 0, 0, tiled=True, axis_index_groups=groups)
    )


def halved_total(parts):
    n = lax.axis_size("row")
    reach = n // 2
    groups = [list(range(reach)), list(range(reach, n))]
    mine = swap(parts, groups)
    here = call(half_sum_kernel, shape(*parts.shape[1:]), [VMEM])(mine)
    there = near(lax.ppermute(here, "row", [(i, (i + reach) % n) for i in range(n)]))
    both = call(join_kernel, shape(*parts.shape), [VMEM, VMEM])(here, there)
    return swap(both, groups)


def body(snapshot, weights, block_home, plan):
    rows = snapshot.shape[0]
    width = weights.shape[1]
    reach = lax.axis_size("row") // 2
    chunk = sum(chunk_rows(reach, width))
    snap_ahead, snap_behind = both_ways(snapshot)
    plan_ahead, plan_behind = both_ways(plan)
    wide = pltpu.VMEM((4, rows, 2 * width), bf16)
    packed, high, low = call(
        pack_kernel, [shape(reach, chunk, width), wide, wide], [SMEM, VMEM], width=width
    )(far(plan), far(snapshot))
    packed, high, low = call(
        raw_kernel,
        [shape(reach, chunk, width), wide, wide],
        [SMEM] * 3 + [VMEM] * 5,
        {5: 0, 6: 1, 7: 2},
        width=width,
    )(plan, plan_ahead, plan_behind, near(snap_ahead), near(snap_behind), packed, high, low)
    gathered = halved_total(packed)
    tall = 3 * width + tile
    send, turned, spread = call(
        first_kernel,
        [shape(2, tall, width), shape(2, 2 * width, width), shape(2, tile, width)],
        [SMEM, SMEM, VMEM, VMEM],
        width=width,
    )(plan, block_home, weights, gathered)
    received = exchange(send)
    keep = call(stay_kernel, shape(2, tall, width), [VMEM, VMEM, VMEM], width=width)(
        gathered, turned, spread
    )
    block = pltpu.VMEM((2, rows, 2 * width), bf16)
    send, turned, norms, block_high, block_low = call(
        second_kernel,
        [
            shape(2, rows + tile, width),
            shape(2, 2 * width, width),
            shape(2, tile, width),
            block,
            block,
        ],
        [SMEM] + [VMEM] * 5,
        width=width,
    )(plan, keep, received, gathered, high, low)
    arrived = exchange(send)
    kept = call(finish_kernel, shape(2, rows, width), [VMEM, VMEM, VMEM])(
        block_high, block_low, turned
    )
    final, norms = call(
        last_kernel,
        [jax.ShapeDtypeStruct((rows, 4 * width), f32), jax.ShapeDtypeStruct((4, width), f32)],
        [VMEM, VMEM, VMEM],
    )(kept, norms, arrived)
    return final, norms.reshape(4 * width)


def solution(mesh):
    in_specs = (P("row", "pair"), P(), P("pair"), P(None, "pair", None))
    out_specs = (P("row", "pair"), P("pair"))
    return jax.shard_map(body, mesh=mesh, in_specs=in_specs, out_specs=out_specs, check_vma=False)
```

```python
import jax
import jax.numpy as jnp
from jax import lax
from jax.experimental import pallas as pl
from jax.experimental.pallas import tpu as pltpu
from jax.sharding import PartitionSpec as P

epsilon = 1e-06
step_size = 4.0
newton_turns = 5
tile = 8
grant = 16 * 1024 * 1024
f32 = jnp.float32
bf16 = jnp.bfloat16

VMEM = pl.BlockSpec(memory_space=pltpu.VMEM)
SMEM = pl.BlockSpec(memory_space=pltpu.SMEM)


def split(x):
    high = x.astype(bf16)
    return high, (x - high.astype(f32)).astype(bf16)


def dot(a, b, da, db):
    return lax.dot_general(a, b, (((da,), (db,)), ((), ())), preferred_element_type=f32)


def dot3(a, b, da, db):
    return dot(a[0], b[0], da, db) + (dot(a[0], b[1], da, db) + dot(a[1], b[0], da, db))


def iotas(n):
    return (
        lax.broadcasted_iota(jnp.int32, (n, n), 0),
        lax.broadcasted_iota(jnp.int32, (n, n), 1),
    )


def column(row):
    n = row.shape[1]
    return jnp.transpose(jnp.broadcast_to(row, (n, n)))


def start_rotation(gram, row_weight):
    n = gram.shape[0]
    i, j = iotas(n)
    same = i == j
    held = jnp.where(same, gram, 0.0)
    inv_row = lax.rsqrt(jnp.sum(held, axis=0, keepdims=True) + epsilon)
    inv_col = lax.rsqrt(jnp.sum(held, axis=1, keepdims=True) + epsilon)
    corr = gram * inv_col * inv_row
    skew = step_size * corr * (column(row_weight) - row_weight)
    bound = 1.0 + jnp.max(jnp.sum(jnp.abs(skew), axis=0, keepdims=True), axis=1, keepdims=True)
    return jnp.where(same, 1.0, 0.0) + skew * (1.0 / bound)


def rotations(grams, row_weights, fillers=()):
    n = grams[0].shape[0]
    i, j = iotas(n)
    same = i == j
    diag15 = jnp.where(same, 1.5, 0.0)
    diag05 = jnp.where(same, 0.5, 0.0)
    current = [start_rotation(g, w) for g, w in zip(grams, row_weights)]
    for turn in range(newton_turns - 1):
        parts = [split(x) for x in current]
        inner = [dot3(p, p, 1, 1) for p in parts]
        if turn < len(fillers):
            fillers[turn]()
        if turn < newton_turns - 2:
            turns = [split(diag15 - 0.5 * y) for y in inner]
            current = [dot3(p, t, 1, 0) for p, t in zip(parts, turns)]
    small = [diag05 - 0.5 * y for y in inner]
    low = [e.astype(bf16) for e in small]
    squared = [dot(e, e, 1, 0) for e in low]
    rest = [(diag15 + (2.5 * e + u)).astype(bf16) for e, u in zip(small, squared)]
    fixes = [
        (e + dot(u.astype(bf16), r, 1, 0)).astype(bf16) for e, u, r in zip(small, squared, rest)
    ]
    return [x + dot(p[0], f, 1, 0) for x, p, f in zip(current, parts, fixes)]


def sizes(n, rows):
    return max(tile, rows // n)


def chunk_rows(reach, width):
    return sizes(reach, 4 * width), sizes(reach, 8 * width), tile


def pair_of(snap, plan, p, width):
    return jnp.concatenate(
        [
            snap[:, pl.ds(pl.multiple_of(plan[0, 0, 2 * p + h] * width, width), width)]
            for h in range(2)
        ],
        axis=1,
    )


def pack_kernel(plan, snap, out, high, low, plan_out, *, width):
    reach = out.shape[0]
    t = lax.broadcasted_iota(jnp.int32, plan.shape, 0)
    k = lax.broadcasted_iota(jnp.int32, plan.shape, 2)
    copied = jnp.zeros(plan.shape, jnp.int32)
    for a in range(plan.shape[0]):
        for b in range(plan.shape[2]):
            copied = jnp.where((t == a) & (k == b), plan[a, 0, b], copied)
    plan_out[...] = copied
    main, raw, _ = chunk_rows(reach, width)
    i, j = iotas(width)
    held = []
    diags = []
    for p in range(2):
        parts = split(pair_of(snap, plan, p, width))
        high[1 + p] = parts[0]
        low[1 + p] = parts[1]
        gram = dot3(parts, parts, 0, 0)
        upper = gram[:width, :width]
        lower = gram[width:, width:]
        held.append(gram[:width, width:])
        held.append(jnp.where(i <= j, upper, lower))
        diags.append(jnp.sum(jnp.where(i == j, lower, 0.0), axis=0, keepdims=True))
    extra = jnp.concatenate(diags + [jnp.zeros((tile - 2, width), f32)], axis=0)
    for c in range(reach):
        start = c * main
        out[c, :main, :] = held[start // width][start % width : start % width + main]
        out[c, main + raw :, :] = extra if c == 0 else jnp.zeros((tile, width), f32)


def raw_kernel(
    plan, plan_ahead, plan_behind, ahead, behind, packed, own_high, own_low, out, high, low, *, width
):
    del packed, own_high, own_low
    for s, snap, order, p in [(0, ahead, plan_ahead, 0), (3, behind, plan_behind, 1)]:
        parts = split(pair_of(snap, order, p, width))
        high[s] = parts[0]
        low[s] = parts[1]
    reach = out.shape[0]
    main, raw, _ = chunk_rows(reach, width)
    crosses = []
    for r in range(2):
        a, b = [plan[1, 0, 2 * r + h] for h in range(2)]
        crosses.append(dot3((high[b], low[b]), (high[a], low[a]), 0, 0))
    tall = 2 * width
    for c in range(reach):
        block, at = divmod(c * raw, tall)
        out[c, main : main + raw, :] = half(crosses[block // 2], block % 2)[at : at + raw]


def half(x, h):
    width = x.shape[1] // 2
    return x[:, h * width : (h + 1) * width]


def added(values):
    while len(values) > 1:
        values = [a + b for a, b in zip(values[0::2], values[1::2])] + (
            [values[-1]] if len(values) % 2 else []
        )
    return values[0]


def half_sum_kernel(parts, out):
    out[...] = added([parts[c] for c in range(parts.shape[0])])


def join_kernel(here, there, out):
    value = here[...] + there[...]
    for c in range(out.shape[0]):
        out[c] = value


def unpack(gathered, p, width):
    main, raw, _ = chunk_rows(gathered.shape[0], width)
    per = width // main
    cross, both = [
        jnp.concatenate(
            [gathered[(2 * p + q) * per + c, :main, :] for c in range(per)], axis=0
        )
        for q in range(2)
    ]
    i, j = iotas(width)
    flipped = jnp.transpose(both)
    diag_b = gathered[0, main + raw + p : main + raw + p + 1, :]
    upper = jnp.where(i <= j, both, flipped)
    lower = jnp.where(i > j, both, jnp.where(i == j, diag_b, flipped))
    return whole(upper, cross, jnp.transpose(cross), lower)


def unpack_raw(gathered, r, width):
    main, raw, _ = chunk_rows(gathered.shape[0], width)
    per = 2 * width // raw
    return jnp.concatenate(
        [
            jnp.concatenate(
                [
                    gathered[(2 * r + h) * per + c, main : main + raw, :]
                    for c in range(per)
                ],
                axis=0,
            )
            for h in range(2)
        ],
        axis=1,
    )


def whole(upper, cross, flipped, lower):
    return jnp.concatenate(
        [
            jnp.concatenate([upper, cross], axis=1),
            jnp.concatenate([flipped, lower], axis=1),
        ],
        axis=0,
    )


def own_gram(gram, q):
    return dot3(q, split(dot3(split(gram), q, 1, 0)), 0, 0)


def first_kernel(plan, home, weights, gathered, send, turned, spread, *, width):
    tall = 2 * width
    grams, spreads = [], []
    for p in range(2):
        grams.append(unpack(gathered, p, width))
        spreads.append(
            jnp.concatenate(
                [weights[pl.ds(home[plan[0, 0, 2 * p + h]], 1), :] for h in range(2)], axis=1
            )
        )
    turns = rotations(grams, spreads)
    for p in range(2):
        q = half(turns[p], p)
        send[p, :tall, :] = q
        send[p, tall : tall + width, :] = own_gram(grams[p], split(q))
        send[p, tall + width :, :] = jnp.broadcast_to(half(spreads[p], p), (tile, width))
        spread[p] = jnp.broadcast_to(half(spreads[p], 1 - p), (tile, width))
        turned[p] = half(turns[p], 1 - p)


def stay_kernel(gathered, turned, spread, keep, *, width):
    tall = 2 * width
    for p in range(2):
        q = turned[p]
        keep[p, :tall, :] = q
        keep[p, tall : tall + width, :] = own_gram(unpack(gathered, p, width), split(q))
        keep[p, tall + width :, :] = spread[p]


def slot_value(s, received, keep, cut):
    values = [received[0, cut, :], keep[0, cut, :], keep[1, cut, :], received[1, cut, :]]
    return jnp.where(s < 2, jnp.where(s == 0, *values[:2]), jnp.where(s == 2, *values[2:]))


def second_kernel(
    plan, keep, received, gathered, high, low, send, turned, norms, block_high, block_low, *, width
):
    tall = 2 * width
    rows = high.shape[1]
    grams, spreads, fillers = [], [], []

    def filler(r, h, s, q):
        def block():
            at = slice(h * width, (h + 1) * width)
            value = split(dot3((high[s], low[s]), q, 1, 0))
            block_high[r, :, at] = value[0]
            block_low[r, :, at] = value[1]

        return block

    for r in range(2):
        order = [plan[1, 0, 2 * r + h] for h in range(2)]
        first, second = [split(slot_value(s, received, keep, slice(0, tall))) for s in order]
        moved = dot3(split(unpack_raw(gathered, r, width)), first, 1, 0)
        flipped = dot3(second, split(moved), 0, 0)
        own = [slot_value(s, received, keep, slice(tall, tall + width)) for s in order]
        grams.append(whole(own[0], jnp.transpose(flipped), flipped, own[1]))
        wide = [
            slot_value(s, received, keep, slice(tall + width, tall + width + 1)) for s in order
        ]
        spreads.append(jnp.concatenate(wide, axis=1))
        fillers += [filler(r, h, s, q) for h, (s, q) in enumerate(zip(order, (first, second)))]
    turns = rotations(grams, spreads, fillers)
    for p in range(2):
        q = split(turns[p])
        send[p, :rows, :] = dot3(
            (block_high[p], block_low[p]), [half(x, p) for x in q], 1, 0
        )
        moved = dot3(split(grams[p]), q, 1, 0)
        squares = jnp.sum(turns[p] * moved, axis=0, keepdims=True)
        lengths = jnp.sqrt(squares)
        send[p, rows:, :] = jnp.broadcast_to(half(lengths, p), (tile, width))
        norms[p] = jnp.broadcast_to(half(lengths, 1 - p), (tile, width))
        turned[p] = half(turns[p], 1 - p)


def finish_kernel(high, low, turned, kept):
    for p in range(2):
        kept[p] = dot3((high[p], low[p]), split(turned[p]), 1, 0)


def last_kernel(kept, norms_here, received, final, norms):
    rows, width = kept.shape[1], kept.shape[2]
    order = [received[0, :rows, :], kept[0], kept[1], received[1, :rows, :]]
    lengths = [received[0, rows:, :], norms_here[0], norms_here[1], received[1, rows:, :]]
    for s in range(4):
        final[:, s * width : (s + 1) * width] = order[s]
        norms[s : s + 1, :] = lengths[s][:1]


def near(x):
    return pltpu.with_memory_space_constraint(x, pltpu.VMEM)


def far(x):
    return pltpu.with_memory_space_constraint(x, pltpu.HBM)


def call(kernel, outs, specs, aliases=None, **static):
    def run(*refs):
        kernel(*refs, **static)

    return pl.pallas_call(
        run,
        out_shape=outs,
        in_specs=specs,
        out_specs=jax.tree.map(lambda _: VMEM, outs),
        input_output_aliases=aliases or {},
        compiler_params=pltpu.CompilerParams(vmem_limit_bytes=grant),
        name=kernel.__name__,
    )


def shape(*dims):
    return pltpu.VMEM(dims, f32)


def routes():
    count = lax.axis_size("pair")
    ahead = [((i - 1) % count, i) for i in range(count)]
    behind = [((i + 1) % count, i) for i in range(count)]
    return ahead, behind, sorted(ahead) == sorted(behind)


def both_ways(x):
    ahead, behind, alike = routes()
    first = lax.ppermute(x, "pair", ahead)
    return first, first if alike else lax.ppermute(x, "pair", behind)


def exchange(send):
    ahead, behind, alike = routes()
    if alike:
        return near(lax.ppermute(send, "pair", ahead))
    return jnp.stack(
        [lax.ppermute(send[0], "pair", ahead), lax.ppermute(send[1], "pair", behind)]
    )


def swap(parts, groups=None):
    return near(
        lax.all_to_all(parts, "row", 0, 0, tiled=True, axis_index_groups=groups)
    )


def halved_total(parts):
    n = lax.axis_size("row")
    reach = n // 2
    groups = [list(range(reach)), list(range(reach, n))]
    mine = swap(parts, groups)
    here = call(half_sum_kernel, shape(*parts.shape[1:]), [VMEM])(mine)
    there = near(lax.ppermute(here, "row", [(i, (i + reach) % n) for i in range(n)]))
    both = call(join_kernel, shape(*parts.shape), [VMEM, VMEM])(here, there)
    return swap(both, groups)


def body(snapshot, weights, block_home, plan):
    rows = snapshot.shape[0]
    width = weights.shape[1]
    reach = lax.axis_size("row") // 2
    chunk = sum(chunk_rows(reach, width))
    snap_ahead, snap_behind = both_ways(snapshot)
    plan_ahead, plan_behind = both_ways(plan)
    wide = pltpu.VMEM((4, rows, 2 * width), bf16)
    packed, high, low, plan = call(
        pack_kernel,
        [shape(reach, chunk, width), wide, wide, pltpu.VMEM(plan.shape, plan.dtype)],
        [SMEM, VMEM],
        width=width,
    )(far(plan), far(snapshot))
    packed, high, low = call(
        raw_kernel,
        [shape(reach, chunk, width), wide, wide],
        [SMEM] * 3 + [VMEM] * 5,
        {5: 0, 6: 1, 7: 2},
        width=width,
    )(plan, plan_ahead, plan_behind, near(snap_ahead), near(snap_behind), packed, high, low)
    gathered = halved_total(packed)
    tall = 3 * width + tile
    send, turned, spread = call(
        first_kernel,
        [shape(2, tall, width), shape(2, 2 * width, width), shape(2, tile, width)],
        [SMEM, SMEM, VMEM, VMEM],
        width=width,
    )(plan, block_home, weights, gathered)
    received = exchange(send)
    keep = call(stay_kernel, shape(2, tall, width), [VMEM, VMEM, VMEM], width=width)(
        gathered, turned, spread
    )
    block = pltpu.VMEM((2, rows, 2 * width), bf16)
    send, turned, norms, block_high, block_low = call(
        second_kernel,
        [
            shape(2, rows + tile, width),
            shape(2, 2 * width, width),
            shape(2, tile, width),
            block,
            block,
        ],
        [SMEM] + [VMEM] * 5,
        width=width,
    )(plan, keep, received, gathered, high, low)
    arrived = exchange(send)
    kept = call(finish_kernel, shape(2, rows, width), [VMEM, VMEM, VMEM])(
        block_high, block_low, turned
    )
    final, norms = call(
        last_kernel,
        [jax.ShapeDtypeStruct((rows, 4 * width), f32), jax.ShapeDtypeStruct((4, width), f32)],
        [VMEM, VMEM, VMEM],
    )(kept, norms, arrived)
    return final, norms.reshape(4 * width)


def solution(mesh):
    in_specs = (P("row", "pair"), P(), P("pair"), P(None, "pair", None))
    out_specs = (P("row", "pair"), P("pair"))
    return jax.shard_map(body, mesh=mesh, in_specs=in_specs, out_specs=out_specs, check_vma=False)
```

```python
import jax
import jax.numpy as jnp
from jax import lax
from jax.experimental import pallas as pl
from jax.experimental.pallas import tpu as pltpu
from jax.sharding import PartitionSpec as P

epsilon = 1e-06
step_size = 4.0
newton_turns = 5
tile = 8
grant = 16 * 1024 * 1024
f32 = jnp.float32
bf16 = jnp.bfloat16

VMEM = pl.BlockSpec(memory_space=pltpu.VMEM)
SMEM = pl.BlockSpec(memory_space=pltpu.SMEM)


def split(x):
    high = x.astype(bf16)
    return high, (x - high.astype(f32)).astype(bf16)


def dot(a, b, da, db):
    return lax.dot_general(a, b, (((da,), (db,)), ((), ())), preferred_element_type=f32)


def dot3(a, b, da, db):
    return dot(a[0], b[0], da, db) + (dot(a[0], b[1], da, db) + dot(a[1], b[0], da, db))


def outer(a):
    cross = dot(a[1], a[0], 1, 1)
    return dot(a[0], a[0], 1, 1) + (cross + jnp.transpose(cross))


def iotas(n):
    return (
        lax.broadcasted_iota(jnp.int32, (n, n), 0),
        lax.broadcasted_iota(jnp.int32, (n, n), 1),
    )


def column(row):
    n = row.shape[1]
    return jnp.transpose(jnp.broadcast_to(row, (n, n)))


def start_rotation(gram, row_weight):
    n = gram.shape[0]
    i, j = iotas(n)
    same = i == j
    held = jnp.where(same, gram, 0.0)
    inv_row = lax.rsqrt(jnp.sum(held, axis=0, keepdims=True) + epsilon)
    inv_col = lax.rsqrt(jnp.sum(held, axis=1, keepdims=True) + epsilon)
    corr = gram * inv_col * inv_row
    skew = step_size * corr * (column(row_weight) - row_weight)
    bound = 1.0 + jnp.max(jnp.sum(jnp.abs(skew), axis=0, keepdims=True), axis=1, keepdims=True)
    return jnp.where(same, 1.0, 0.0) + skew * (1.0 / bound)


def rotations(grams, row_weights, fillers=()):
    n = grams[0].shape[0]
    i, j = iotas(n)
    same = i == j
    diag15 = jnp.where(same, 1.5, 0.0)
    diag05 = jnp.where(same, 0.5, 0.0)
    current = [start_rotation(g, w) for g, w in zip(grams, row_weights)]
    for turn in range(newton_turns - 1):
        parts = [split(x) for x in current]
        inner = [outer(p) for p in parts]
        if turn < len(fillers):
            fillers[turn]()
        if turn < newton_turns - 2:
            turns = [split(diag15 - 0.5 * y) for y in inner]
            current = [dot3(p, t, 1, 0) for p, t in zip(parts, turns)]
    small = [diag05 - 0.5 * y for y in inner]
    low = [e.astype(bf16) for e in small]
    squared = [dot(e, e, 1, 0) for e in low]
    rest = [(diag15 + (2.5 * e + u)).astype(bf16) for e, u in zip(small, squared)]
    fixes = [
        (e + dot(u.astype(bf16), r, 1, 0)).astype(bf16) for e, u, r in zip(small, squared, rest)
    ]
    return [x + dot(p[0], f, 1, 0) for x, p, f in zip(current, parts, fixes)]


def sizes(n, rows):
    return max(tile, rows // n)


def chunk_rows(reach, width):
    return sizes(reach, 4 * width), sizes(reach, 8 * width), tile


def pair_of(snap, plan, p, width):
    return jnp.concatenate(
        [
            snap[:, pl.ds(pl.multiple_of(plan[0, 0, 2 * p + h] * width, width), width)]
            for h in range(2)
        ],
        axis=1,
    )


def pack_kernel(plan, home, weights, snap, out, high, low, plan_out, spread, *, width):
    reach = out.shape[0]
    t = lax.broadcasted_iota(jnp.int32, plan.shape, 0)
    k = lax.broadcasted_iota(jnp.int32, plan.shape, 2)
    copied = jnp.zeros(plan.shape, jnp.int32)
    for a in range(plan.shape[0]):
        for b in range(plan.shape[2]):
            copied = jnp.where((t == a) & (k == b), plan[a, 0, b], copied)
    plan_out[...] = copied
    for p in range(2):
        row = jnp.concatenate(
            [weights[pl.ds(home[plan[0, 0, 2 * p + h]], 1), :] for h in range(2)], axis=1
        )
        spread[p] = jnp.broadcast_to(row, (tile, 2 * width))
    main, raw, _ = chunk_rows(reach, width)
    i, j = iotas(width)
    held = []
    diags = []
    for p in range(2):
        parts = split(pair_of(snap, plan, p, width))
        high[1 + p] = parts[0]
        low[1 + p] = parts[1]
        gram = dot3(parts, parts, 0, 0)
        upper = gram[:width, :width]
        lower = gram[width:, width:]
        held.append(gram[:width, width:])
        held.append(jnp.where(i <= j, upper, lower))
        diags.append(jnp.sum(jnp.where(i == j, lower, 0.0), axis=0, keepdims=True))
    extra = jnp.concatenate(diags + [jnp.zeros((tile - 2, width), f32)], axis=0)
    for c in range(reach):
        start = c * main
        out[c, :main, :] = held[start // width][start % width : start % width + main]
        out[c, main + raw :, :] = extra if c == 0 else jnp.zeros((tile, width), f32)


def raw_kernel(
    plan, plan_ahead, plan_behind, ahead, behind, packed, own_high, own_low, out, high, low, *, width
):
    del packed, own_high, own_low
    plan, plan_ahead, plan_behind = plan[...], plan_ahead[...], plan_behind[...]
    for s, snap, order, p in [(0, ahead, plan_ahead, 0), (3, behind, plan_behind, 1)]:
        parts = split(pair_of(snap, order, p, width))
        high[s] = parts[0]
        low[s] = parts[1]
    reach = out.shape[0]
    main, raw, _ = chunk_rows(reach, width)
    crosses = []
    for r in range(2):
        a, b = [plan[1, 0, 2 * r + h] for h in range(2)]
        crosses.append(dot3((high[b], low[b]), (high[a], low[a]), 0, 0))
    tall = 2 * width
    for c in range(reach):
        block, at = divmod(c * raw, tall)
        out[c, main : main + raw, :] = half(crosses[block // 2], block % 2)[at : at + raw]


def half(x, h):
    width = x.shape[1] // 2
    return x[:, h * width : (h + 1) * width]


def added(values):
    while len(values) > 1:
        values = [a + b for a, b in zip(values[0::2], values[1::2])] + (
            [values[-1]] if len(values) % 2 else []
        )
    return values[0]


def half_sum_kernel(parts, out):
    out[...] = added([parts[c] for c in range(parts.shape[0])])


def join_kernel(here, there, out):
    value = here[...] + there[...]
    for c in range(out.shape[0]):
        out[c] = value


def unpack(gathered, p, width):
    main, raw, _ = chunk_rows(gathered.shape[0], width)
    per = width // main
    cross, both = [
        jnp.concatenate(
            [gathered[(2 * p + q) * per + c, :main, :] for c in range(per)], axis=0
        )
        for q in range(2)
    ]
    i, j = iotas(width)
    flipped = jnp.transpose(both)
    diag_b = gathered[0, main + raw + p : main + raw + p + 1, :]
    upper = jnp.where(i <= j, both, flipped)
    lower = jnp.where(i > j, both, jnp.where(i == j, diag_b, flipped))
    return whole(upper, cross, jnp.transpose(cross), lower)


def unpack_raw(gathered, r, width):
    main, raw, _ = chunk_rows(gathered.shape[0], width)
    per = 2 * width // raw
    return jnp.concatenate(
        [
            jnp.concatenate(
                [
                    gathered[(2 * r + h) * per + c, main : main + raw, :]
                    for c in range(per)
                ],
                axis=0,
            )
            for h in range(2)
        ],
        axis=1,
    )


def whole(upper, cross, flipped, lower):
    return jnp.concatenate(
        [
            jnp.concatenate([upper, cross], axis=1),
            jnp.concatenate([flipped, lower], axis=1),
        ],
        axis=0,
    )


def own_gram(gram, q):
    return dot3(q, split(dot3(split(gram), q, 1, 0)), 0, 0)


def first_kernel(spread, gathered, send, turned, *, width):
    tall = 2 * width
    grams, spreads = [], []
    for p in range(2):
        grams.append(unpack(gathered, p, width))
        spreads.append(spread[p, :1, :])
    turns = rotations(grams, spreads)
    for p in range(2):
        q = half(turns[p], p)
        send[p, :tall, :] = q
        send[p, tall : tall + width, :] = own_gram(grams[p], split(q))
        send[p, tall + width :, :] = jnp.broadcast_to(half(spreads[p], p), (tile, width))
        turned[p] = half(turns[p], 1 - p)


def stay_kernel(gathered, turned, spread, keep, *, width):
    tall = 2 * width
    for p in range(2):
        q = turned[p]
        keep[p, :tall, :] = q
        keep[p, tall : tall + width, :] = own_gram(unpack(gathered, p, width), split(q))
        keep[p, tall + width :, :] = half(spread[p], 1 - p)


def slot_value(s, received, keep, cut):
    values = [received[0, cut, :], keep[0, cut, :], keep[1, cut, :], received[1, cut, :]]
    return jnp.where(s < 2, jnp.where(s == 0, *values[:2]), jnp.where(s == 2, *values[2:]))


def second_kernel(
    plan, keep, received, gathered, high, low, send, turned, norms, block_high, block_low, *, width
):
    tall = 2 * width
    rows = high.shape[1]
    plan = plan[...]
    grams, spreads, fillers = [], [], []

    def filler(r, h, s, q):
        def block():
            at = slice(h * width, (h + 1) * width)
            value = split(dot3((high[s], low[s]), q, 1, 0))
            block_high[r, :, at] = value[0]
            block_low[r, :, at] = value[1]

        return block

    for r in range(2):
        order = [plan[1, 0, 2 * r + h] for h in range(2)]
        first, second = [split(slot_value(s, received, keep, slice(0, tall))) for s in order]
        moved = dot3(split(unpack_raw(gathered, r, width)), first, 1, 0)
        flipped = dot3(second, split(moved), 0, 0)
        own = [slot_value(s, received, keep, slice(tall, tall + width)) for s in order]
        grams.append(whole(own[0], jnp.transpose(flipped), flipped, own[1]))
        wide = [
            slot_value(s, received, keep, slice(tall + width, tall + width + 1)) for s in order
        ]
        spreads.append(jnp.concatenate(wide, axis=1))
        fillers += [filler(r, h, s, q) for h, (s, q) in enumerate(zip(order, (first, second)))]
    turns = rotations(grams, spreads, fillers)
    for p in range(2):
        q = split(turns[p])
        send[p, :rows, :] = dot3(
            (block_high[p], block_low[p]), [half(x, p) for x in q], 1, 0
        )
        moved = dot3(split(grams[p]), q, 1, 0)
        squares = jnp.sum(turns[p] * moved, axis=0, keepdims=True)
        lengths = jnp.sqrt(squares)
        send[p, rows:, :] = jnp.broadcast_to(half(lengths, p), (tile, width))
        norms[p] = jnp.broadcast_to(half(lengths, 1 - p), (tile, width))
        turned[p] = half(turns[p], 1 - p)


def finish_kernel(high, low, turned, kept):
    for p in range(2):
        kept[p] = dot3((high[p], low[p]), split(turned[p]), 1, 0)


def last_kernel(kept, norms_here, received, final, norms):
    rows, width = kept.shape[1], kept.shape[2]
    order = [received[0, :rows, :], kept[0], kept[1], received[1, :rows, :]]
    lengths = [received[0, rows:, :], norms_here[0], norms_here[1], received[1, rows:, :]]
    for s in range(4):
        final[:, s * width : (s + 1) * width] = order[s]
        norms[s : s + 1, :] = lengths[s][:1]


def near(x):
    return pltpu.with_memory_space_constraint(x, pltpu.VMEM)


def far(x):
    return pltpu.with_memory_space_constraint(x, pltpu.HBM)


def call(kernel, outs, specs, aliases=None, **static):
    def run(*refs):
        kernel(*refs, **static)

    return pl.pallas_call(
        run,
        out_shape=outs,
        in_specs=specs,
        out_specs=jax.tree.map(lambda _: VMEM, outs),
        input_output_aliases=aliases or {},
        compiler_params=pltpu.CompilerParams(vmem_limit_bytes=grant),
        name=kernel.__name__,
    )


def shape(*dims):
    return pltpu.VMEM(dims, f32)


def routes():
    count = lax.axis_size("pair")
    ahead = [((i - 1) % count, i) for i in range(count)]
    behind = [((i + 1) % count, i) for i in range(count)]
    return ahead, behind, sorted(ahead) == sorted(behind)


def both_ways(x):
    ahead, behind, alike = routes()
    first = lax.ppermute(x, "pair", ahead)
    return first, first if alike else lax.ppermute(x, "pair", behind)


def exchange(send):
    ahead, behind, alike = routes()
    if alike:
        return near(lax.ppermute(send, "pair", ahead))
    return jnp.stack(
        [lax.ppermute(send[0], "pair", ahead), lax.ppermute(send[1], "pair", behind)]
    )


def swap(parts, groups=None):
    return near(
        lax.all_to_all(parts, "row", 0, 0, tiled=True, axis_index_groups=groups)
    )


def halved_total(parts):
    n = lax.axis_size("row")
    reach = n // 2
    groups = [list(range(reach)), list(range(reach, n))]
    mine = swap(parts, groups)
    here = call(half_sum_kernel, shape(*parts.shape[1:]), [VMEM])(mine)
    there = near(lax.ppermute(here, "row", [(i, (i + reach) % n) for i in range(n)]))
    both = call(join_kernel, shape(*parts.shape), [VMEM, VMEM])(here, there)
    return swap(both, groups)


def body(snapshot, weights, block_home, plan):
    rows = snapshot.shape[0]
    width = weights.shape[1]
    reach = lax.axis_size("row") // 2
    chunk = sum(chunk_rows(reach, width))
    snap_ahead, snap_behind = both_ways(snapshot)
    plan_ahead, plan_behind = both_ways(plan)
    wide = pltpu.VMEM((4, rows, 2 * width), bf16)
    packed, high, low, plan, spread = call(
        pack_kernel,
        [
            shape(reach, chunk, width),
            wide,
            wide,
            pltpu.VMEM(plan.shape, plan.dtype),
            shape(2, tile, 2 * width),
        ],
        [SMEM, SMEM, VMEM, VMEM],
        width=width,
    )(far(plan), far(block_home), far(weights), far(snapshot))
    packed, high, low = call(
        raw_kernel,
        [shape(reach, chunk, width), wide, wide],
        [VMEM] * 8,
        {5: 0, 6: 1, 7: 2},
        width=width,
    )(plan, near(plan_ahead), near(plan_behind), near(snap_ahead), near(snap_behind), packed, high, low)
    gathered = halved_total(packed)
    tall = 3 * width + tile
    send, turned = call(
        first_kernel,
        [shape(2, tall, width), shape(2, 2 * width, width)],
        [VMEM, VMEM],
        width=width,
    )(spread, gathered)
    received = exchange(send)
    keep = call(stay_kernel, shape(2, tall, width), [VMEM, VMEM, VMEM], width=width)(
        gathered, turned, spread
    )
    block = pltpu.VMEM((2, rows, 2 * width), bf16)
    send, turned, norms, block_high, block_low = call(
        second_kernel,
        [
            shape(2, rows + tile, width),
            shape(2, 2 * width, width),
            shape(2, tile, width),
            block,
            block,
        ],
        [VMEM] * 6,
        width=width,
    )(plan, keep, received, gathered, high, low)
    arrived = exchange(send)
    kept = call(finish_kernel, shape(2, rows, width), [VMEM, VMEM, VMEM])(
        block_high, block_low, turned
    )
    final, norms = call(
        last_kernel,
        [jax.ShapeDtypeStruct((rows, 4 * width), f32), jax.ShapeDtypeStruct((4, width), f32)],
        [VMEM, VMEM, VMEM],
    )(kept, norms, arrived)
    return final, norms.reshape(4 * width)


def solution(mesh):
    in_specs = (P("row", "pair"), P(), P("pair"), P(None, "pair", None))
    out_specs = (P("row", "pair"), P("pair"))
    return jax.shard_map(body, mesh=mesh, in_specs=in_specs, out_specs=out_specs, check_vma=False)
```

```python
import jax
import jax.numpy as jnp
from jax import lax
from jax.experimental import pallas as pl
from jax.experimental.pallas import tpu as pltpu
from jax.sharding import PartitionSpec as P

epsilon = 1e-06
step_size = 4.0
newton_turns = 5
tile = 8
grant = 16 * 1024 * 1024
f32 = jnp.float32
bf16 = jnp.bfloat16

VMEM = pl.BlockSpec(memory_space=pltpu.VMEM)
SMEM = pl.BlockSpec(memory_space=pltpu.SMEM)


def split(x):
    high = x.astype(bf16)
    return high, (x - high.astype(f32)).astype(bf16)


def dot(a, b, da, db):
    return lax.dot_general(a, b, (((da,), (db,)), ((), ())), preferred_element_type=f32)


def dot3(a, b, da, db):
    return dot(a[0], b[0], da, db) + (dot(a[0], b[1], da, db) + dot(a[1], b[0], da, db))


def outer(a):
    cross = dot(a[1], a[0], 1, 1)
    return dot(a[0], a[0], 1, 1) + (cross + jnp.transpose(cross))


def iotas(n):
    return (
        lax.broadcasted_iota(jnp.int32, (n, n), 0),
        lax.broadcasted_iota(jnp.int32, (n, n), 1),
    )


def column(row):
    n = row.shape[1]
    return jnp.transpose(jnp.broadcast_to(row, (n, n)))


def start_rotation(gram, row_weight):
    n = gram.shape[0]
    i, j = iotas(n)
    same = i == j
    held = jnp.where(same, gram, 0.0)
    inv_row = lax.rsqrt(jnp.sum(held, axis=0, keepdims=True) + epsilon)
    inv_col = lax.rsqrt(jnp.sum(held, axis=1, keepdims=True) + epsilon)
    corr = gram * inv_col * inv_row
    skew = step_size * corr * (column(row_weight) - row_weight)
    bound = 1.0 + jnp.max(jnp.sum(jnp.abs(skew), axis=0, keepdims=True), axis=1, keepdims=True)
    return jnp.where(same, 1.0, 0.0) + skew * (1.0 / bound)


def rotations(grams, row_weights, fillers=()):
    n = grams[0].shape[0]
    i, j = iotas(n)
    same = i == j
    diag15 = jnp.where(same, 1.5, 0.0)
    diag05 = jnp.where(same, 0.5, 0.0)
    current = [start_rotation(g, w) for g, w in zip(grams, row_weights)]
    for turn in range(newton_turns - 1):
        parts = [split(x) for x in current]
        inner = [outer(p) for p in parts]
        if turn < len(fillers):
            fillers[turn]()
        if turn < newton_turns - 2:
            turns = [split(diag15 - 0.5 * y) for y in inner]
            current = [dot3(p, t, 1, 0) for p, t in zip(parts, turns)]
    small = [diag05 - 0.5 * y for y in inner]
    low = [e.astype(bf16) for e in small]
    squared = [dot(e, e, 1, 0) for e in low]
    rest = [(diag15 + (2.5 * e + u)).astype(bf16) for e, u in zip(small, squared)]
    fixes = [
        (e + dot(u.astype(bf16), r, 1, 0)).astype(bf16) for e, u, r in zip(small, squared, rest)
    ]
    return [x + dot(p[0], f, 1, 0) for x, p, f in zip(current, parts, fixes)]


def sizes(n, rows):
    return max(tile, rows // n)


def chunk_rows(reach, width):
    return sizes(reach, 4 * width), sizes(reach, 8 * width), tile


def pair_of(snap, plan, p, width):
    return jnp.concatenate(
        [
            snap[:, pl.ds(pl.multiple_of(plan[0, 0, 2 * p + h] * width, width), width)]
            for h in range(2)
        ],
        axis=1,
    )


def pack_kernel(plan, home, weights, snap, out, high, low, plan_out, spread, *, width):
    reach = out.shape[0]
    t = lax.broadcasted_iota(jnp.int32, plan.shape, 0)
    k = lax.broadcasted_iota(jnp.int32, plan.shape, 2)
    copied = jnp.zeros(plan.shape, jnp.int32)
    for a in range(plan.shape[0]):
        for b in range(plan.shape[2]):
            copied = jnp.where((t == a) & (k == b), plan[a, 0, b], copied)
    plan_out[...] = copied
    for p in range(2):
        row = jnp.concatenate(
            [weights[pl.ds(home[plan[0, 0, 2 * p + h]], 1), :] for h in range(2)], axis=1
        )
        spread[p] = jnp.broadcast_to(row, (tile, 2 * width))
    main, raw, _ = chunk_rows(reach, width)
    i, j = iotas(width)
    held = []
    diags = []
    for p in range(2):
        parts = split(pair_of(snap, plan, p, width))
        high[1 + p] = parts[0]
        low[1 + p] = parts[1]
        gram = dot3(parts, parts, 0, 0)
        upper = gram[:width, :width]
        lower = gram[width:, width:]
        held.append(gram[:width, width:])
        held.append(jnp.where(i <= j, upper, lower))
        diags.append(jnp.sum(jnp.where(i == j, lower, 0.0), axis=0, keepdims=True))
    extra = jnp.concatenate(diags + [jnp.zeros((tile - 2, width), f32)], axis=0)
    for c in range(reach):
        start = c * main
        out[c, :main, :] = held[start // width][start % width : start % width + main]
        out[c, main + raw :, :] = extra if c == 0 else jnp.zeros((tile, width), f32)


def raw_kernel(
    plan, plan_ahead, plan_behind, ahead, behind, packed, own_high, own_low, out, high, low, *, width
):
    del packed, own_high, own_low
    plan, plan_ahead, plan_behind = plan[...], plan_ahead[...], plan_behind[...]
    for s, snap, order, p in [(0, ahead, plan_ahead, 0), (3, behind, plan_behind, 1)]:
        parts = split(pair_of(snap, order, p, width))
        high[s] = parts[0]
        low[s] = parts[1]
    reach = out.shape[0]
    main, raw, _ = chunk_rows(reach, width)
    crosses = []
    for r in range(2):
        a, b = [plan[1, 0, 2 * r + h] for h in range(2)]
        crosses.append(dot3((high[b], low[b]), (high[a], low[a]), 0, 0))
    tall = 2 * width
    for c in range(reach):
        block, at = divmod(c * raw, tall)
        out[c, main : main + raw, :] = half(crosses[block // 2], block % 2)[at : at + raw]


def half(x, h):
    width = x.shape[1] // 2
    return x[:, h * width : (h + 1) * width]


def added(values):
    while len(values) > 1:
        values = [a + b for a, b in zip(values[0::2], values[1::2])] + (
            [values[-1]] if len(values) % 2 else []
        )
    return values[0]


def half_sum_kernel(parts, out):
    out[...] = added([parts[c] for c in range(parts.shape[0])])


def join_kernel(here, there, out):
    value = here[...] + there[...]
    for c in range(out.shape[0]):
        out[c] = value


def unpack(gathered, p, width):
    main, raw, _ = chunk_rows(gathered.shape[0], width)
    per = width // main
    cross, both = [
        jnp.concatenate(
            [gathered[(2 * p + q) * per + c, :main, :] for c in range(per)], axis=0
        )
        for q in range(2)
    ]
    i, j = iotas(width)
    flipped = jnp.transpose(both)
    diag_b = gathered[0, main + raw + p : main + raw + p + 1, :]
    upper = jnp.where(i <= j, both, flipped)
    lower = jnp.where(i > j, both, jnp.where(i == j, diag_b, flipped))
    return whole(upper, cross, jnp.transpose(cross), lower)


def unpack_raw(gathered, r, width):
    main, raw, _ = chunk_rows(gathered.shape[0], width)
    per = 2 * width // raw
    return jnp.concatenate(
        [
            jnp.concatenate(
                [
                    gathered[(2 * r + h) * per + c, main : main + raw, :]
                    for c in range(per)
                ],
                axis=0,
            )
            for h in range(2)
        ],
        axis=1,
    )


def whole(upper, cross, flipped, lower):
    return jnp.concatenate(
        [
            jnp.concatenate([upper, cross], axis=1),
            jnp.concatenate([flipped, lower], axis=1),
        ],
        axis=0,
    )


def own_gram(gram, q):
    return dot3(q, split(dot3(split(gram), q, 1, 0)), 0, 0)


def first_kernel(spread, gathered, send, turned, *, width):
    tall = 2 * width
    grams, spreads = [], []
    for p in range(2):
        grams.append(unpack(gathered, p, width))
        spreads.append(spread[p, :1, :])
    turns = rotations(grams, spreads)
    for p in range(2):
        q = half(turns[p], p)
        send[p, :tall, :] = q
        send[p, tall : tall + width, :] = own_gram(grams[p], split(q))
        send[p, tall + width :, :] = jnp.broadcast_to(half(spreads[p], p), (tile, width))
        turned[p] = half(turns[p], 1 - p)


def stay_kernel(gathered, turned, spread, keep, *, width):
    tall = 2 * width
    for p in range(2):
        q = turned[p]
        keep[p, :tall, :] = q
        keep[p, tall : tall + width, :] = own_gram(unpack(gathered, p, width), split(q))
        keep[p, tall + width :, :] = half(spread[p], 1 - p)


def slot_value(s, received, keep, cut):
    values = [received[0, cut, :], keep[0, cut, :], keep[1, cut, :], received[1, cut, :]]
    return jnp.where(s < 2, jnp.where(s == 0, *values[:2]), jnp.where(s == 2, *values[2:]))


def second_kernel(
    plan, keep, received, gathered, high, low, send, turned, norms, block_high, block_low, *, width
):
    tall = 2 * width
    rows = high.shape[1]
    plan = plan[...]
    grams, spreads, fillers = [], [], []

    def filler(r, h, s, q):
        def block():
            at = slice(h * width, (h + 1) * width)
            value = split(dot3((high[s], low[s]), q, 1, 0))
            block_high[r, :, at] = value[0]
            block_low[r, :, at] = value[1]

        return block

    for r in range(2):
        order = [plan[1, 0, 2 * r + h] for h in range(2)]
        first, second = [split(slot_value(s, received, keep, slice(0, tall))) for s in order]
        moved = dot3(split(unpack_raw(gathered, r, width)), first, 1, 0)
        flipped = dot3(second, split(moved), 0, 0)
        own = [slot_value(s, received, keep, slice(tall, tall + width)) for s in order]
        grams.append(whole(own[0], jnp.transpose(flipped), flipped, own[1]))
        wide = [
            slot_value(s, received, keep, slice(tall + width, tall + width + 1)) for s in order
        ]
        spreads.append(jnp.concatenate(wide, axis=1))
        fillers += [filler(r, h, s, q) for h, (s, q) in enumerate(zip(order, (first, second)))]
    turns = rotations(grams, spreads, fillers)
    for p in range(2):
        q = split(turns[p])
        send[p, :rows, :] = dot3(
            (block_high[p], block_low[p]), [half(x, p) for x in q], 1, 0
        )
        moved = dot3(split(grams[p]), q, 1, 0)
        squares = jnp.sum(turns[p] * moved, axis=0, keepdims=True)
        lengths = jnp.sqrt(squares)
        send[p, rows:, :] = jnp.broadcast_to(half(lengths, p), (tile, width))
        norms[p] = jnp.broadcast_to(half(lengths, 1 - p), (tile, width))
        turned[p] = half(turns[p], 1 - p)


def finish_kernel(high, low, turned, kept):
    for p in range(2):
        kept[p] = dot3((high[p], low[p]), split(turned[p]), 1, 0)


def last_kernel(kept, norms_here, received, final, norms):
    rows, width = kept.shape[1], kept.shape[2]
    order = [received[0, :rows, :], kept[0], kept[1], received[1, :rows, :]]
    lengths = [received[0, rows:, :], norms_here[0], norms_here[1], received[1, rows:, :]]
    for s in range(4):
        final[:, s * width : (s + 1) * width] = order[s]
        norms[s : s + 1, :] = lengths[s][:1]


def near(x):
    return pltpu.with_memory_space_constraint(x, pltpu.VMEM)


def far(x):
    return pltpu.with_memory_space_constraint(x, pltpu.HBM)


def call(kernel, outs, specs, aliases=None, **static):
    def run(*refs):
        kernel(*refs, **static)

    return pl.pallas_call(
        run,
        out_shape=outs,
        in_specs=specs,
        out_specs=jax.tree.map(lambda _: VMEM, outs),
        input_output_aliases=aliases or {},
        compiler_params=pltpu.CompilerParams(vmem_limit_bytes=grant),
        name=kernel.__name__,
    )


def shape(*dims):
    return pltpu.VMEM(dims, f32)


def routes():
    count = lax.axis_size("pair")
    ahead = [((i - 1) % count, i) for i in range(count)]
    behind = [((i + 1) % count, i) for i in range(count)]
    return ahead, behind, sorted(ahead) == sorted(behind)


def both_ways(x):
    ahead, behind, alike = routes()
    first = lax.ppermute(x, "pair", ahead)
    return first, first if alike else lax.ppermute(x, "pair", behind)


def exchange(send):
    ahead, behind, alike = routes()
    if alike:
        return near(lax.ppermute(send, "pair", ahead))
    return jnp.stack(
        [lax.ppermute(send[0], "pair", ahead), lax.ppermute(send[1], "pair", behind)]
    )


def swap(parts, groups=None):
    return near(
        lax.all_to_all(parts, "row", 0, 0, tiled=True, axis_index_groups=groups)
    )


def halved_total(parts):
    n = lax.axis_size("row")
    reach = n // 2
    quarter = reach // 2
    mirror = [(3 - i // quarter) * quarter + i % quarter for i in range(n)]
    groups = [list(range(reach)), mirror[:reach]]
    mine = swap(parts, groups)
    here = call(half_sum_kernel, shape(*parts.shape[1:]), [VMEM])(mine)
    there = near(lax.ppermute(here, "row", list(enumerate(mirror))))
    both = call(join_kernel, shape(*parts.shape), [VMEM, VMEM])(here, there)
    return swap(both, groups)


def body(snapshot, weights, block_home, plan):
    rows = snapshot.shape[0]
    width = weights.shape[1]
    reach = lax.axis_size("row") // 2
    chunk = sum(chunk_rows(reach, width))
    snap_ahead, snap_behind = both_ways(snapshot)
    plan_ahead, plan_behind = both_ways(plan)
    wide = pltpu.VMEM((4, rows, 2 * width), bf16)
    packed, high, low, plan, spread = call(
        pack_kernel,
        [
            shape(reach, chunk, width),
            wide,
            wide,
            pltpu.VMEM(plan.shape, plan.dtype),
            shape(2, tile, 2 * width),
        ],
        [SMEM, SMEM, VMEM, VMEM],
        width=width,
    )(far(plan), far(block_home), far(weights), far(snapshot))
    packed, high, low = call(
        raw_kernel,
        [shape(reach, chunk, width), wide, wide],
        [VMEM] * 8,
        {5: 0, 6: 1, 7: 2},
        width=width,
    )(plan, near(plan_ahead), near(plan_behind), near(snap_ahead), near(snap_behind), packed, high, low)
    gathered = halved_total(packed)
    tall = 3 * width + tile
    send, turned = call(
        first_kernel,
        [shape(2, tall, width), shape(2, 2 * width, width)],
        [VMEM, VMEM],
        width=width,
    )(spread, gathered)
    received = exchange(send)
    keep = call(stay_kernel, shape(2, tall, width), [VMEM, VMEM, VMEM], width=width)(
        gathered, turned, spread
    )
    block = pltpu.VMEM((2, rows, 2 * width), bf16)
    send, turned, norms, block_high, block_low = call(
        second_kernel,
        [
            shape(2, rows + tile, width),
            shape(2, 2 * width, width),
            shape(2, tile, width),
            block,
            block,
        ],
        [VMEM] * 6,
        width=width,
    )(plan, keep, received, gathered, high, low)
    arrived = exchange(send)
    kept = call(finish_kernel, shape(2, rows, width), [VMEM, VMEM, VMEM])(
        block_high, block_low, turned
    )
    final, norms = call(
        last_kernel,
        [jax.ShapeDtypeStruct((rows, 4 * width), f32), jax.ShapeDtypeStruct((4, width), f32)],
        [VMEM, VMEM, VMEM],
    )(kept, norms, arrived)
    return final, norms.reshape(4 * width)


def solution(mesh):
    in_specs = (P("row", "pair"), P(), P("pair"), P(None, "pair", None))
    out_specs = (P("row", "pair"), P("pair"))
    return jax.shard_map(body, mesh=mesh, in_specs=in_specs, out_specs=out_specs, check_vma=False)
```

```python
import jax
import jax.numpy as jnp
from jax import lax
from jax.experimental import pallas as pl
from jax.experimental.pallas import tpu as pltpu
from jax.sharding import PartitionSpec as P

epsilon = 1e-06
step_size = 4.0
newton_turns = 5
tile = 8
grant = 16 * 1024 * 1024
f32 = jnp.float32
bf16 = jnp.bfloat16

VMEM = pl.BlockSpec(memory_space=pltpu.VMEM)
SMEM = pl.BlockSpec(memory_space=pltpu.SMEM)


def split(x):
    high = x.astype(bf16)
    return high, (x - high.astype(f32)).astype(bf16)


def dot(a, b, da, db):
    return lax.dot_general(a, b, (((da,), (db,)), ((), ())), preferred_element_type=f32)


def dot3(a, b, da, db):
    return dot(a[0], b[0], da, db) + (dot(a[0], b[1], da, db) + dot(a[1], b[0], da, db))


def outer(a):
    cross = dot(a[1], a[0], 1, 1)
    return dot(a[0], a[0], 1, 1) + (cross + jnp.transpose(cross))


def iotas(n):
    return (
        lax.broadcasted_iota(jnp.int32, (n, n), 0),
        lax.broadcasted_iota(jnp.int32, (n, n), 1),
    )


def column(row):
    n = row.shape[1]
    return jnp.transpose(jnp.broadcast_to(row, (n, n)))


def start_rotation(gram, row_weight):
    n = gram.shape[0]
    i, j = iotas(n)
    same = i == j
    held = jnp.where(same, gram, 0.0)
    inv_row = lax.rsqrt(jnp.maximum(jnp.sum(held, axis=0, keepdims=True), 0.0) + epsilon)
    inv_col = lax.rsqrt(jnp.maximum(jnp.sum(held, axis=1, keepdims=True), 0.0) + epsilon)
    corr = gram * inv_col * inv_row
    skew = step_size * corr * (column(row_weight) - row_weight)
    bound = 1.0 + jnp.max(jnp.sum(jnp.abs(skew), axis=0, keepdims=True), axis=1, keepdims=True)
    return jnp.where(same, 1.0, 0.0) + skew * (1.0 / bound)


def rotations(grams, row_weights, fillers=()):
    n = grams[0].shape[0]
    i, j = iotas(n)
    same = i == j
    diag15 = jnp.where(same, 1.5, 0.0)
    diag05 = jnp.where(same, 0.5, 0.0)
    current = [start_rotation(g, w) for g, w in zip(grams, row_weights)]
    for turn in range(newton_turns - 1):
        parts = [split(x) for x in current]
        inner = [outer(p) for p in parts]
        if turn < len(fillers):
            fillers[turn]()
        if turn < newton_turns - 2:
            turns = [split(diag15 - 0.5 * y) for y in inner]
            current = [dot3(p, t, 1, 0) for p, t in zip(parts, turns)]
    small = [diag05 - 0.5 * y for y in inner]
    low = [e.astype(bf16) for e in small]
    squared = [dot(e, e, 1, 0) for e in low]
    rest = [(diag15 + (2.5 * e + u)).astype(bf16) for e, u in zip(small, squared)]
    fixes = [
        (e + dot(u.astype(bf16), r, 1, 0)).astype(bf16) for e, u, r in zip(small, squared, rest)
    ]
    return [x + dot(p[0], f, 1, 0) for x, p, f in zip(current, parts, fixes)]


def sizes(n, rows):
    return max(tile, rows // n)


def chunk_rows(reach, width):
    return sizes(reach, 4 * width), sizes(reach, 8 * width), tile


def pair_of(snap, plan, p, width):
    return jnp.concatenate(
        [
            snap[:, pl.ds(pl.multiple_of(plan[0, 0, 2 * p + h] * width, width), width)]
            for h in range(2)
        ],
        axis=1,
    )


def pack_kernel(plan, home, weights, snap, out, high, low, plan_out, spread, *, width):
    reach = out.shape[0]
    t = lax.broadcasted_iota(jnp.int32, plan.shape, 0)
    k = lax.broadcasted_iota(jnp.int32, plan.shape, 2)
    copied = jnp.zeros(plan.shape, jnp.int32)
    for a in range(plan.shape[0]):
        for b in range(plan.shape[2]):
            copied = jnp.where((t == a) & (k == b), plan[a, 0, b], copied)
    plan_out[...] = copied
    for p in range(2):
        row = jnp.concatenate(
            [weights[pl.ds(home[plan[0, 0, 2 * p + h]], 1), :] for h in range(2)], axis=1
        )
        spread[p] = jnp.broadcast_to(row, (tile, 2 * width))
    main, raw, _ = chunk_rows(reach, width)
    i, j = iotas(width)
    held = []
    diags = []
    for p in range(2):
        parts = split(pair_of(snap, plan, p, width))
        high[1 + p] = parts[0]
        low[1 + p] = parts[1]
        gram = dot3(parts, parts, 0, 0)
        upper = gram[:width, :width]
        lower = gram[width:, width:]
        held.append(gram[:width, width:])
        held.append(jnp.where(i <= j, upper, lower))
        diags.append(jnp.sum(jnp.where(i == j, lower, 0.0), axis=0, keepdims=True))
    extra = jnp.concatenate(diags + [jnp.zeros((tile - 2, width), f32)], axis=0)
    for c in range(reach):
        start = c * main
        out[c, :main, :] = held[start // width][start % width : start % width + main]
        out[c, main + raw :, :] = extra if c == 0 else jnp.zeros((tile, width), f32)


def raw_kernel(
    plan, plan_ahead, plan_behind, ahead, behind, packed, own_high, own_low, out, high, low, *, width
):
    del packed, own_high, own_low
    plan, plan_ahead, plan_behind = plan[...], plan_ahead[...], plan_behind[...]
    for s, snap, order, p in [(0, ahead, plan_ahead, 0), (3, behind, plan_behind, 1)]:
        parts = split(pair_of(snap, order, p, width))
        high[s] = parts[0]
        low[s] = parts[1]
    reach = out.shape[0]
    main, raw, _ = chunk_rows(reach, width)
    crosses = []
    for r in range(2):
        a, b = [plan[1, 0, 2 * r + h] for h in range(2)]
        crosses.append(dot3((high[b], low[b]), (high[a], low[a]), 0, 0))
    tall = 2 * width
    for c in range(reach):
        block, at = divmod(c * raw, tall)
        out[c, main : main + raw, :] = half(crosses[block // 2], block % 2)[at : at + raw]


def half(x, h):
    width = x.shape[1] // 2
    return x[:, h * width : (h + 1) * width]


def added(values):
    while len(values) > 1:
        values = [a + b for a, b in zip(values[0::2], values[1::2])] + (
            [values[-1]] if len(values) % 2 else []
        )
    return values[0]


def half_sum_kernel(parts, out):
    out[...] = added([parts[c] for c in range(parts.shape[0])])


def join_kernel(here, there, out):
    value = here[...] + there[...]
    for c in range(out.shape[0]):
        out[c] = value


def unpack(gathered, p, width):
    main, raw, _ = chunk_rows(gathered.shape[0], width)
    per = width // main
    cross, both = [
        jnp.concatenate(
            [gathered[(2 * p + q) * per + c, :main, :] for c in range(per)], axis=0
        )
        for q in range(2)
    ]
    i, j = iotas(width)
    flipped = jnp.transpose(both)
    diag_b = gathered[0, main + raw + p : main + raw + p + 1, :]
    upper = jnp.where(i <= j, both, flipped)
    lower = jnp.where(i > j, both, jnp.where(i == j, diag_b, flipped))
    return whole(upper, cross, jnp.transpose(cross), lower)


def unpack_raw(gathered, r, width):
    main, raw, _ = chunk_rows(gathered.shape[0], width)
    per = 2 * width // raw
    return jnp.concatenate(
        [
            jnp.concatenate(
                [
                    gathered[(2 * r + h) * per + c, main : main + raw, :]
                    for c in range(per)
                ],
                axis=0,
            )
            for h in range(2)
        ],
        axis=1,
    )


def whole(upper, cross, flipped, lower):
    return jnp.concatenate(
        [
            jnp.concatenate([upper, cross], axis=1),
            jnp.concatenate([flipped, lower], axis=1),
        ],
        axis=0,
    )


def own_gram(gram, q):
    return dot3(q, split(dot3(split(gram), q, 1, 0)), 0, 0)


def first_kernel(spread, gathered, send, turned, *, width):
    tall = 2 * width
    grams, spreads = [], []
    for p in range(2):
        grams.append(unpack(gathered, p, width))
        spreads.append(spread[p, :1, :])
    turns = rotations(grams, spreads)
    for p in range(2):
        q = half(turns[p], p)
        send[p, :tall, :] = q
        send[p, tall : tall + width, :] = own_gram(grams[p], split(q))
        send[p, tall + width :, :] = jnp.broadcast_to(half(spreads[p], p), (tile, width))
        turned[p] = half(turns[p], 1 - p)


def stay_kernel(gathered, turned, spread, keep, raw_high, raw_low, *, width):
    tall = 2 * width
    for p in range(2):
        raw_high[p], raw_low[p] = split(unpack_raw(gathered, p, width))
        q = turned[p]
        keep[p, :tall, :] = q
        keep[p, tall : tall + width, :] = own_gram(unpack(gathered, p, width), split(q))
        keep[p, tall + width :, :] = half(spread[p], 1 - p)


def slot_value(s, received, keep, cut):
    values = [received[0, cut, :], keep[0, cut, :], keep[1, cut, :], received[1, cut, :]]
    return jnp.where(s < 2, jnp.where(s == 0, *values[:2]), jnp.where(s == 2, *values[2:]))


def second_kernel(
    plan,
    keep,
    received,
    raw_high,
    raw_low,
    high,
    low,
    send,
    turned,
    held,
    block_high,
    block_low,
    *,
    width,
):
    tall = 2 * width
    rows = high.shape[1]
    plan = plan[...]
    grams, spreads, fillers = [], [], []

    def filler(r, h, s, q):
        def block():
            at = slice(h * width, (h + 1) * width)
            value = split(dot3((high[s], low[s]), q, 1, 0))
            block_high[r, :, at] = value[0]
            block_low[r, :, at] = value[1]

        return block

    for r in range(2):
        order = [plan[1, 0, 2 * r + h] for h in range(2)]
        first, second = [split(slot_value(s, received, keep, slice(0, tall))) for s in order]
        moved = dot3((raw_high[r], raw_low[r]), first, 1, 0)
        flipped = dot3(second, split(moved), 0, 0)
        own = [slot_value(s, received, keep, slice(tall, tall + width)) for s in order]
        grams.append(whole(own[0], jnp.transpose(flipped), flipped, own[1]))
        wide = [
            slot_value(s, received, keep, slice(tall + width, tall + width + 1)) for s in order
        ]
        spreads.append(jnp.concatenate(wide, axis=1))
        fillers += [filler(r, h, s, q) for h, (s, q) in enumerate(zip(order, (first, second)))]
    turns = rotations(grams, spreads, fillers)
    for p in range(2):
        turn = half(turns[p], p)
        send[p, :rows, :] = dot3((block_high[p], block_low[p]), split(turn), 1, 0)
        send[p, rows:, :] = lengths(grams[p], turn)
        held[p] = grams[p]
        turned[p] = half(turns[p], 1 - p)


def lengths(gram, turn):
    squares = jnp.sum(turn * dot3(split(gram), split(turn), 1, 0), axis=0, keepdims=True)
    return jnp.broadcast_to(jnp.sqrt(jnp.maximum(squares, 0.0)), (tile, turn.shape[1]))


def finish_kernel(high, low, turned, grams, kept, norms):
    for p in range(2):
        kept[p] = dot3((high[p], low[p]), split(turned[p]), 1, 0)
        norms[p] = lengths(grams[p], turned[p])


def last_kernel(kept, norms_here, received, final, norms):
    rows, width = kept.shape[1], kept.shape[2]
    order = [received[0, :rows, :], kept[0], kept[1], received[1, :rows, :]]
    lengths = [received[0, rows:, :], norms_here[0], norms_here[1], received[1, rows:, :]]
    for s in range(4):
        final[:, s * width : (s + 1) * width] = order[s]
        norms[s : s + 1, :] = lengths[s][:1]


def near(x):
    return pltpu.with_memory_space_constraint(x, pltpu.VMEM)


def far(x):
    return pltpu.with_memory_space_constraint(x, pltpu.HBM)


def call(kernel, outs, specs, aliases=None, **static):
    def run(*refs):
        kernel(*refs, **static)

    return pl.pallas_call(
        run,
        out_shape=outs,
        in_specs=specs,
        out_specs=jax.tree.map(lambda _: VMEM, outs),
        input_output_aliases=aliases or {},
        compiler_params=pltpu.CompilerParams(vmem_limit_bytes=grant),
        name=kernel.__name__,
    )


def shape(*dims):
    return pltpu.VMEM(dims, f32)


def routes():
    count = lax.axis_size("pair")
    ahead = [((i - 1) % count, i) for i in range(count)]
    behind = [((i + 1) % count, i) for i in range(count)]
    return ahead, behind, sorted(ahead) == sorted(behind)


def both_ways(x):
    ahead, behind, alike = routes()
    first = lax.ppermute(x, "pair", ahead)
    return first, first if alike else lax.ppermute(x, "pair", behind)


def exchange(send):
    ahead, behind, alike = routes()
    if alike:
        return near(lax.ppermute(send, "pair", ahead))
    return jnp.stack(
        [lax.ppermute(send[0], "pair", ahead), lax.ppermute(send[1], "pair", behind)]
    )


def swap(parts, groups=None):
    return near(
        lax.all_to_all(parts, "row", 0, 0, tiled=True, axis_index_groups=groups)
    )


def halved_total(parts):
    n = lax.axis_size("row")
    reach = n // 2
    quarter = reach // 2
    mirror = [(3 - i // quarter) * quarter + i % quarter for i in range(n)]
    groups = [list(range(reach)), mirror[:reach]]
    mine = swap(parts, groups)
    here = call(half_sum_kernel, shape(*parts.shape[1:]), [VMEM])(mine)
    there = near(lax.ppermute(here, "row", list(enumerate(mirror))))
    both = call(join_kernel, shape(*parts.shape), [VMEM, VMEM])(here, there)
    return swap(both, groups)


def body(snapshot, weights, block_home, plan):
    rows = snapshot.shape[0]
    width = weights.shape[1]
    reach = lax.axis_size("row") // 2
    chunk = sum(chunk_rows(reach, width))
    snap_ahead, snap_behind = both_ways(snapshot)
    plan_ahead, plan_behind = both_ways(plan)
    wide = pltpu.VMEM((4, rows, 2 * width), bf16)
    packed, high, low, plan, spread = call(
        pack_kernel,
        [
            shape(reach, chunk, width),
            wide,
            wide,
            pltpu.VMEM(plan.shape, plan.dtype),
            shape(2, tile, 2 * width),
        ],
        [SMEM, SMEM, VMEM, VMEM],
        width=width,
    )(far(plan), far(block_home), far(weights), far(snapshot))
    packed, high, low = call(
        raw_kernel,
        [shape(reach, chunk, width), wide, wide],
        [VMEM] * 8,
        {5: 0, 6: 1, 7: 2},
        width=width,
    )(plan, near(plan_ahead), near(plan_behind), near(snap_ahead), near(snap_behind), packed, high, low)
    gathered = halved_total(packed)
    tall = 3 * width + tile
    send, turned = call(
        first_kernel,
        [shape(2, tall, width), shape(2, 2 * width, width)],
        [VMEM, VMEM],
        width=width,
    )(spread, gathered)
    received = exchange(send)
    square = pltpu.VMEM((2, 2 * width, 2 * width), bf16)
    keep, raw_high, raw_low = call(
        stay_kernel, [shape(2, tall, width), square, square], [VMEM, VMEM, VMEM], width=width
    )(gathered, turned, spread)
    block = pltpu.VMEM((2, rows, 2 * width), bf16)
    send, turned, held, block_high, block_low = call(
        second_kernel,
        [
            shape(2, rows + tile, width),
            shape(2, 2 * width, width),
            shape(2, 2 * width, 2 * width),
            block,
            block,
        ],
        [VMEM] * 7,
        width=width,
    )(plan, keep, received, raw_high, raw_low, high, low)
    arrived = exchange(send)
    kept, norms = call(
        finish_kernel, [shape(2, rows, width), shape(2, tile, width)], [VMEM] * 4
    )(block_high, block_low, turned, held)
    final, norms = call(
        last_kernel,
        [jax.ShapeDtypeStruct((rows, 4 * width), f32), jax.ShapeDtypeStruct((4, width), f32)],
        [VMEM, VMEM, VMEM],
    )(kept, norms, arrived)
    return final, norms.reshape(4 * width)


def solution(mesh):
    in_specs = (P("row", "pair"), P(), P("pair"), P(None, "pair", None))
    out_specs = (P("row", "pair"), P("pair"))
    return jax.shard_map(body, mesh=mesh, in_specs=in_specs, out_specs=out_specs, check_vma=False)
```

```python
import jax
import jax.numpy as jnp
from jax import lax
from jax.experimental import pallas as pl
from jax.experimental.pallas import tpu as pltpu
from jax.sharding import PartitionSpec as P

epsilon = 1e-06
step_size = 4.0
newton_turns = 5
tile = 8
grant = 16 * 1024 * 1024
f32 = jnp.float32
bf16 = jnp.bfloat16

VMEM = pl.BlockSpec(memory_space=pltpu.VMEM)
SMEM = pl.BlockSpec(memory_space=pltpu.SMEM)


def split(x):
    high = x.astype(bf16)
    return high, (x - high.astype(f32)).astype(bf16)


def dot(a, b, da, db):
    return lax.dot_general(a, b, (((da,), (db,)), ((), ())), preferred_element_type=f32)


def dot3(a, b, da, db):
    return dot(a[0], b[0], da, db) + (dot(a[0], b[1], da, db) + dot(a[1], b[0], da, db))


def outer(a):
    cross = dot(a[1], a[0], 1, 1)
    return dot(a[0], a[0], 1, 1) + (cross + jnp.transpose(cross))


def iotas(n):
    return (
        lax.broadcasted_iota(jnp.int32, (n, n), 0),
        lax.broadcasted_iota(jnp.int32, (n, n), 1),
    )


def column(row):
    n = row.shape[1]
    return jnp.transpose(jnp.broadcast_to(row, (n, n)))


def difference(row_weight):
    return step_size * (column(row_weight) - row_weight)


def start_rotation(gram, apart):
    n = gram.shape[0]
    i, j = iotas(n)
    same = i == j
    held = jnp.where(same, gram, 0.0)
    inv_row = lax.rsqrt(jnp.maximum(jnp.sum(held, axis=0, keepdims=True), 0.0) + epsilon)
    inv_col = lax.rsqrt(jnp.maximum(jnp.sum(held, axis=1, keepdims=True), 0.0) + epsilon)
    corr = gram * inv_col * inv_row
    skew = corr * apart
    bound = 1.0 + jnp.max(jnp.sum(jnp.abs(skew), axis=0, keepdims=True), axis=1, keepdims=True)
    return jnp.where(same, 1.0, 0.0) + skew * (1.0 / bound)


def rotations(grams, aparts, fillers=()):
    n = grams[0].shape[0]
    i, j = iotas(n)
    same = i == j
    diag15 = jnp.where(same, 1.5, 0.0)
    diag05 = jnp.where(same, 0.5, 0.0)
    current = [start_rotation(g, a) for g, a in zip(grams, aparts)]
    for turn in range(newton_turns - 1):
        parts = [split(x) for x in current]
        inner = [outer(p) for p in parts]
        if turn < len(fillers):
            fillers[turn]()
        if turn < newton_turns - 2:
            turns = [split(diag15 - 0.5 * y) for y in inner]
            current = [dot3(p, t, 1, 0) for p, t in zip(parts, turns)]
    small = [diag05 - 0.5 * y for y in inner]
    low = [e.astype(bf16) for e in small]
    squared = [dot(e, e, 1, 0) for e in low]
    rest = [(diag15 + (2.5 * e + u)).astype(bf16) for e, u in zip(small, squared)]
    fixes = [
        (e + dot(u.astype(bf16), r, 1, 0)).astype(bf16) for e, u, r in zip(small, squared, rest)
    ]
    return [x + dot(p[0], f, 1, 0) for x, p, f in zip(current, parts, fixes)]


def sizes(n, rows):
    return max(tile, rows // n)


def chunk_rows(reach, width):
    return sizes(reach, 4 * width), sizes(reach, 8 * width), tile


def pair_of(snap, plan, p, width):
    return jnp.concatenate(
        [
            snap[:, pl.ds(pl.multiple_of(plan[0, 0, 2 * p + h] * width, width), width)]
            for h in range(2)
        ],
        axis=1,
    )


def pack_kernel(plan, home, weights, snap, out, high, low, plan_out, spread, *, width):
    reach = out.shape[0]
    t = lax.broadcasted_iota(jnp.int32, plan.shape, 0)
    k = lax.broadcasted_iota(jnp.int32, plan.shape, 2)
    copied = jnp.zeros(plan.shape, jnp.int32)
    for a in range(plan.shape[0]):
        for b in range(plan.shape[2]):
            copied = jnp.where((t == a) & (k == b), plan[a, 0, b], copied)
    plan_out[...] = copied
    for p in range(2):
        row = jnp.concatenate(
            [weights[pl.ds(home[plan[0, 0, 2 * p + h]], 1), :] for h in range(2)], axis=1
        )
        spread[p] = jnp.broadcast_to(row, (tile, 2 * width))
    main, raw, _ = chunk_rows(reach, width)
    i, j = iotas(width)
    held = []
    diags = []
    for p in range(2):
        parts = split(pair_of(snap, plan, p, width))
        high[1 + p] = parts[0]
        low[1 + p] = parts[1]
        gram = dot3(parts, parts, 0, 0)
        upper = gram[:width, :width]
        lower = gram[width:, width:]
        held.append(gram[:width, width:])
        held.append(jnp.where(i <= j, upper, lower))
        diags.append(jnp.sum(jnp.where(i == j, lower, 0.0), axis=0, keepdims=True))
    extra = jnp.concatenate(diags + [jnp.zeros((tile - 2, width), f32)], axis=0)
    for c in range(reach):
        start = c * main
        out[c, :main, :] = held[start // width][start % width : start % width + main]
        out[c, main + raw :, :] = extra if c == 0 else jnp.zeros((tile, width), f32)


def raw_kernel(
    plan, plan_ahead, plan_behind, ahead, behind, packed, own_high, own_low, out, high, low, *, width
):
    del packed, own_high, own_low
    plan, plan_ahead, plan_behind = plan[...], plan_ahead[...], plan_behind[...]
    for s, snap, order, p in [(0, ahead, plan_ahead, 0), (3, behind, plan_behind, 1)]:
        parts = split(pair_of(snap, order, p, width))
        high[s] = parts[0]
        low[s] = parts[1]
    reach = out.shape[0]
    main, raw, _ = chunk_rows(reach, width)
    crosses = []
    for r in range(2):
        a, b = [plan[1, 0, 2 * r + h] for h in range(2)]
        crosses.append(dot3((high[b], low[b]), (high[a], low[a]), 0, 0))
    tall = 2 * width
    for c in range(reach):
        block, at = divmod(c * raw, tall)
        out[c, main : main + raw, :] = half(crosses[block // 2], block % 2)[at : at + raw]


def half(x, h):
    width = x.shape[1] // 2
    return x[:, h * width : (h + 1) * width]


def added(values):
    while len(values) > 1:
        values = [a + b for a, b in zip(values[0::2], values[1::2])] + (
            [values[-1]] if len(values) % 2 else []
        )
    return values[0]


def half_sum_kernel(parts, out):
    out[...] = added([parts[c] for c in range(parts.shape[0])])


def join_kernel(here, there, aparts, out):
    del aparts
    value = here[...] + there[...]
    for c in range(out.shape[0]):
        out[c] = value


def unpack(gathered, p, width):
    main, raw, _ = chunk_rows(gathered.shape[0], width)
    per = width // main
    cross, both = [
        jnp.concatenate(
            [gathered[(2 * p + q) * per + c, :main, :] for c in range(per)], axis=0
        )
        for q in range(2)
    ]
    i, j = iotas(width)
    flipped = jnp.transpose(both)
    diag_b = gathered[0, main + raw + p : main + raw + p + 1, :]
    upper = jnp.where(i <= j, both, flipped)
    lower = jnp.where(i > j, both, jnp.where(i == j, diag_b, flipped))
    return whole(upper, cross, jnp.transpose(cross), lower)


def unpack_raw(gathered, r, width):
    main, raw, _ = chunk_rows(gathered.shape[0], width)
    per = 2 * width // raw
    return jnp.concatenate(
        [
            jnp.concatenate(
                [
                    gathered[(2 * r + h) * per + c, main : main + raw, :]
                    for c in range(per)
                ],
                axis=0,
            )
            for h in range(2)
        ],
        axis=1,
    )


def whole(upper, cross, flipped, lower):
    return jnp.concatenate(
        [
            jnp.concatenate([upper, cross], axis=1),
            jnp.concatenate([flipped, lower], axis=1),
        ],
        axis=0,
    )


def own_gram(gram, q):
    return dot3(q, split(dot3(split(gram), q, 1, 0)), 0, 0)


def apart_kernel(spread, sums, out):
    del sums
    for p in range(2):
        out[p] = difference(spread[p, :1, :])


def first_kernel(spread, aparts, gathered, send, turned, *, width):
    tall = 2 * width
    grams, spreads = [], []
    for p in range(2):
        grams.append(unpack(gathered, p, width))
        spreads.append(spread[p, :1, :])
    turns = rotations(grams, [aparts[p] for p in range(2)])
    for p in range(2):
        q = half(turns[p], p)
        send[p, :tall, :] = q
        send[p, tall : tall + width, :] = own_gram(grams[p], split(q))
        send[p, tall + width :, :] = jnp.broadcast_to(half(spreads[p], p), (tile, width))
        turned[p] = half(turns[p], 1 - p)


def stay_kernel(gathered, turned, spread, keep, raw_high, raw_low, *, width):
    tall = 2 * width
    for p in range(2):
        raw_high[p], raw_low[p] = split(unpack_raw(gathered, p, width))
        q = turned[p]
        keep[p, :tall, :] = q
        keep[p, tall : tall + width, :] = own_gram(unpack(gathered, p, width), split(q))
        keep[p, tall + width :, :] = half(spread[p], 1 - p)


def slot_value(s, received, keep, cut):
    values = [received[0, cut, :], keep[0, cut, :], keep[1, cut, :], received[1, cut, :]]
    return jnp.where(s < 2, jnp.where(s == 0, *values[:2]), jnp.where(s == 2, *values[2:]))


def second_kernel(
    plan,
    keep,
    received,
    raw_high,
    raw_low,
    high,
    low,
    send,
    turned,
    held,
    block_high,
    block_low,
    *,
    width,
):
    tall = 2 * width
    rows = high.shape[1]
    plan = plan[...]
    grams, spreads, fillers = [], [], []

    def filler(r, h, s, q):
        def block():
            at = slice(h * width, (h + 1) * width)
            value = split(dot3((high[s], low[s]), q, 1, 0))
            block_high[r, :, at] = value[0]
            block_low[r, :, at] = value[1]

        return block

    for r in range(2):
        order = [plan[1, 0, 2 * r + h] for h in range(2)]
        first, second = [split(slot_value(s, received, keep, slice(0, tall))) for s in order]
        moved = dot3((raw_high[r], raw_low[r]), first, 1, 0)
        flipped = dot3(second, split(moved), 0, 0)
        own = [slot_value(s, received, keep, slice(tall, tall + width)) for s in order]
        grams.append(whole(own[0], jnp.transpose(flipped), flipped, own[1]))
        wide = [
            slot_value(s, received, keep, slice(tall + width, tall + width + 1)) for s in order
        ]
        spreads.append(jnp.concatenate(wide, axis=1))
        fillers += [filler(r, h, s, q) for h, (s, q) in enumerate(zip(order, (first, second)))]
    turns = rotations(grams, [difference(w) for w in spreads], fillers)
    for p in range(2):
        turn = half(turns[p], p)
        send[p, :rows, :] = dot3((block_high[p], block_low[p]), split(turn), 1, 0)
        send[p, rows:, :] = lengths(grams[p], turn)
        held[p] = grams[p]
        turned[p] = half(turns[p], 1 - p)


def lengths(gram, turn):
    squares = jnp.sum(turn * dot3(split(gram), split(turn), 1, 0), axis=0, keepdims=True)
    return jnp.broadcast_to(jnp.sqrt(jnp.maximum(squares, 0.0)), (tile, turn.shape[1]))


def finish_kernel(high, low, turned, grams, kept, norms):
    for p in range(2):
        kept[p] = dot3((high[p], low[p]), split(turned[p]), 1, 0)
        norms[p] = lengths(grams[p], turned[p])


def last_kernel(kept, norms_here, received, final, norms):
    rows, width = kept.shape[1], kept.shape[2]
    order = [received[0, :rows, :], kept[0], kept[1], received[1, :rows, :]]
    lengths = [received[0, rows:, :], norms_here[0], norms_here[1], received[1, rows:, :]]
    for s in range(4):
        final[:, s * width : (s + 1) * width] = order[s]
        norms[s : s + 1, :] = lengths[s][:1]


def near(x):
    return pltpu.with_memory_space_constraint(x, pltpu.VMEM)


def far(x):
    return pltpu.with_memory_space_constraint(x, pltpu.HBM)


def call(kernel, outs, specs, aliases=None, **static):
    def run(*refs):
        kernel(*refs, **static)

    return pl.pallas_call(
        run,
        out_shape=outs,
        in_specs=specs,
        out_specs=jax.tree.map(lambda _: VMEM, outs),
        input_output_aliases=aliases or {},
        compiler_params=pltpu.CompilerParams(vmem_limit_bytes=grant),
        name=kernel.__name__,
    )


def shape(*dims):
    return pltpu.VMEM(dims, f32)


def routes():
    count = lax.axis_size("pair")
    ahead = [((i - 1) % count, i) for i in range(count)]
    behind = [((i + 1) % count, i) for i in range(count)]
    return ahead, behind, sorted(ahead) == sorted(behind)


def both_ways(x):
    ahead, behind, alike = routes()
    first = lax.ppermute(x, "pair", ahead)
    return first, first if alike else lax.ppermute(x, "pair", behind)


def exchange(send):
    ahead, behind, alike = routes()
    if alike:
        return near(lax.ppermute(send, "pair", ahead))
    return jnp.stack(
        [lax.ppermute(send[0], "pair", ahead), lax.ppermute(send[1], "pair", behind)]
    )


def swap(parts, groups=None):
    return near(
        lax.all_to_all(parts, "row", 0, 0, tiled=True, axis_index_groups=groups)
    )


def halved_total(parts, spread):
    n = lax.axis_size("row")
    reach, width = n // 2, parts.shape[2]
    quarter = reach // 2
    mirror = [(3 - i // quarter) * quarter + i % quarter for i in range(n)]
    groups = [list(range(reach)), mirror[:reach]]
    mine = swap(parts, groups)
    here = call(half_sum_kernel, shape(*parts.shape[1:]), [VMEM])(mine)
    there = near(lax.ppermute(here, "row", list(enumerate(mirror))))
    side = 2 * width
    aparts = call(apart_kernel, shape(2, side, side), [VMEM, VMEM])(spread, here)
    both = call(join_kernel, shape(*parts.shape), [VMEM] * 3)(here, there, aparts)
    return swap(both, groups), aparts


def body(snapshot, weights, block_home, plan):
    rows = snapshot.shape[0]
    width = weights.shape[1]
    reach = lax.axis_size("row") // 2
    chunk = sum(chunk_rows(reach, width))
    snap_ahead, snap_behind = both_ways(snapshot)
    plan_ahead, plan_behind = both_ways(plan)
    wide = pltpu.VMEM((4, rows, 2 * width), bf16)
    packed, high, low, plan, spread = call(
        pack_kernel,
        [
            shape(reach, chunk, width),
            wide,
            wide,
            pltpu.VMEM(plan.shape, plan.dtype),
            shape(2, tile, 2 * width),
        ],
        [SMEM, SMEM, VMEM, VMEM],
        width=width,
    )(far(plan), far(block_home), far(weights), far(snapshot))
    packed, high, low = call(
        raw_kernel,
        [shape(reach, chunk, width), wide, wide],
        [VMEM] * 8,
        {5: 0, 6: 1, 7: 2},
        width=width,
    )(plan, near(plan_ahead), near(plan_behind), near(snap_ahead), near(snap_behind), packed, high, low)
    gathered, aparts = halved_total(packed, spread)
    tall = 3 * width + tile
    send, turned = call(
        first_kernel,
        [shape(2, tall, width), shape(2, 2 * width, width)],
        [VMEM, VMEM, VMEM],
        width=width,
    )(spread, aparts, gathered)
    received = exchange(send)
    square = pltpu.VMEM((2, 2 * width, 2 * width), bf16)
    keep, raw_high, raw_low = call(
        stay_kernel, [shape(2, tall, width), square, square], [VMEM, VMEM, VMEM], width=width
    )(gathered, turned, spread)
    block = pltpu.VMEM((2, rows, 2 * width), bf16)
    send, turned, held, block_high, block_low = call(
        second_kernel,
        [
            shape(2, rows + tile, width),
            shape(2, 2 * width, width),
            shape(2, 2 * width, 2 * width),
            block,
            block,
        ],
        [VMEM] * 7,
        width=width,
    )(plan, keep, received, raw_high, raw_low, high, low)
    arrived = exchange(send)
    kept, norms = call(
        finish_kernel, [shape(2, rows, width), shape(2, tile, width)], [VMEM] * 4
    )(block_high, block_low, turned, held)
    final, norms = call(
        last_kernel,
        [jax.ShapeDtypeStruct((rows, 4 * width), f32), jax.ShapeDtypeStruct((4, width), f32)],
        [VMEM, VMEM, VMEM],
    )(kept, norms, arrived)
    return final, norms.reshape(4 * width)


def solution(mesh):
    in_specs = (P("row", "pair"), P(), P("pair"), P(None, "pair", None))
    out_specs = (P("row", "pair"), P("pair"))
    return jax.shard_map(body, mesh=mesh, in_specs=in_specs, out_specs=out_specs, check_vma=False)
```
